8 devices in a mesh: dp: 1 (over z), tp: 2 (over y), sp: 4 (over x, core).
Axes of the slice: x: 2, y: 2, z: 1, core: 2. Of those that a mesh axis runs over, the one named last changes fastest.
Arguments:
- hidden: bfloat16 [16, 1536], P('dp')
- k_cache: bfloat16 [16, 8192, 12, 128], P('dp', 'sp', 'tp')
- v_cache: bfloat16 [16, 8192, 12, 128], P('dp', 'sp', 'tp')
- lengths: int32 [16], P('dp')
- rel_table: bfloat16 [8192, 12, 128], P('sp', 'tp')
- u_bias: bfloat16 [12, 128], P('tp')
- w_bias: bfloat16 [12, 128], P('tp')
- g_attn: bfloat16 [1536], replicated
- w_query: bfloat16 [1536, 12, 128], P(None, 'tp')
- w_key: bfloat16 [1536, 12, 128], P(None, 'tp')
- w_value: bfloat16 [1536, 12, 128], P(None, 'tp')
- w_out: bfloat16 [12, 128, 1536], P('tp')
- g_mlp: bfloat16 [1536], replicated
- w_up: bfloat16 [1536, 6144], P(None, 'tp')
- w_down: bfloat16 [6144, 1536], P('tp')
Outputs:
- output: bfloat16 [16, 1536], P('dp')
All inputs are finite; a program needn't handle non-finite values.
Results may differ from the reference program's by a relative error of at most 0.0124729.
Values sent between devices are 32-bit elements.
A program may use at most 1 GiB of HBM per device.

```python
import math
import jax
import jax.numpy as jnp
from jax import lax

BATCH = 16
SMAX = 8192
D = 1536
HEADS = 12
HEAD = 128
FF = 6144
EPS = 1e-6
MASKED = -1e30


def setup_inputs(seed: int = 0, part: int = 0) -> dict:
    base = jax.random.key(seed)
    shared_keys = jax.random.split(base, 11)
    part_keys = jax.random.split(jax.random.fold_in(base, part), 5)
    key_scale = math.sqrt(math.log(SMAX / 32.0) / 4.0)
    cache_shape = (BATCH, SMAX, HEADS, HEAD)
    hidden = jax.random.normal(part_keys[0], (BATCH, D), jnp.float32)
    k_cache = jax.random.normal(part_keys[1], cache_shape, jnp.float32) * key_scale
    v_cache = jax.random.normal(part_keys[2], cache_shape, jnp.float32)
    drawn_len = jax.random.randint(part_keys[3], (BATCH,), SMAX // 8, SMAX)
    full_slot = jax.random.randint(part_keys[4], (), 0, BATCH)
    lengths = jnp.where(jnp.arange(BATCH) == full_slot, SMAX - 1, drawn_len).astype(jnp.int32)
    rel_table = jax.random.normal(shared_keys[0], (SMAX, HEADS, HEAD), jnp.float32) * key_scale
    u_bias = jax.random.normal(shared_keys[1], (HEADS, HEAD), jnp.float32)
    w_bias = jax.random.normal(shared_keys[2], (HEADS, HEAD), jnp.float32)
    g_attn = 1.0 + 0.3 * jax.random.normal(shared_keys[3], (D,), jnp.float32)
    w_query = jax.random.normal(shared_keys[4], (D, HEADS, HEAD), jnp.float32) * D ** -0.5
    w_key = jax.random.normal(shared_keys[5], (D, HEADS, HEAD), jnp.float32) * (2.5 * key_scale * D ** -0.5)
    w_value = jax.random.normal(shared_keys[6], (D, HEADS, HEAD), jnp.float32) * (2.0 * D ** -0.5)
    w_out = jax.random.normal(shared_keys[7], (HEADS, HEAD, D), jnp.float32) * (3.0 * (HEADS * HEAD) ** -0.5)
    g_mlp = 1.0 + 0.3 * jax.random.normal(shared_keys[8], (D,), jnp.float32)
    w_up = jax.random.normal(shared_keys[9], (D, FF), jnp.float32) * D ** -0.5
    w_down = jax.random.normal(shared_keys[10], (FF, D), jnp.float32) * FF ** -0.5
    return {
        'hidden': hidden.astype(jnp.bfloat16),
        'k_cache': k_cache.astype(jnp.bfloat16),
        'v_cache': v_cache.astype(jnp.bfloat16),
        'lengths': lengths,
        'rel_table': rel_table.astype(jnp.bfloat16),
        'u_bias': u_bias.astype(jnp.bfloat16),
        'w_bias': w_bias.astype(jnp.bfloat16),
        'g_attn': g_attn.astype(jnp.bfloat16),
        'w_query': w_query.astype(jnp.bfloat16),
        'w_key': w_key.astype(jnp.bfloat16),
        'w_value': w_value.astype(jnp.bfloat16),
        'w_out': w_out.astype(jnp.bfloat16),
        'g_mlp': g_mlp.astype(jnp.bfloat16),
        'w_up': w_up.astype(jnp.bfloat16),
        'w_down': w_down.astype(jnp.bfloat16),
    }


def rms_norm(tensor, gain):
    wide = tensor.astype(jnp.float32)
    mean_sq = jnp.mean(wide * wide, axis=-1, keepdims=True)
    return (wide * lax.rsqrt(mean_sq + EPS) * gain.astype(jnp.float32)).astype(jnp.bfloat16)


def reference(hidden, k_cache, v_cache, lengths, rel_table, u_bias, w_bias, g_attn, w_query, w_key, w_value, w_out, g_mlp, w_up, w_down):
    normed = rms_norm(hidden, g_attn)
    query_vec = jnp.dot(normed, w_query.reshape(D, HEADS * HEAD), preferred_element_type=jnp.float32).astype(jnp.bfloat16).reshape(BATCH, HEADS, HEAD)
    key_new = jnp.dot(normed, w_key.reshape(D, HEADS * HEAD), preferred_element_type=jnp.float32).astype(jnp.bfloat16).reshape(BATCH, HEADS, HEAD)
    value_new = jnp.dot(normed, w_value.reshape(D, HEADS * HEAD), preferred_element_type=jnp.float32).astype(jnp.bfloat16).reshape(BATCH, HEADS, HEAD)
    positions = jnp.arange(SMAX)
    write_mask = (positions[None, :] == lengths[:, None])[:, :, None, None]
    k_updated = jnp.where(write_mask, key_new[:, None], k_cache)
    v_updated = jnp.where(write_mask, value_new[:, None], v_cache)
    q_content = (query_vec.astype(jnp.float32) + u_bias.astype(jnp.float32)).astype(jnp.bfloat16)
    q_position = (query_vec.astype(jnp.float32) + w_bias.astype(jnp.float32)).astype(jnp.bfloat16)
    rel_wide = rel_table.astype(jnp.float32)

    def attend_one(packed):
        q_cont, q_pos, k_seq, v_seq, length = packed
        content = jnp.einsum('hd,shd->hs', q_cont.astype(jnp.float32), k_seq.astype(jnp.float32))
        by_distance = jnp.einsum('hd,shd->hs', q_pos.astype(jnp.float32), rel_wide)
        distance = length - positions
        relative = by_distance[:, jnp.clip(distance, 0, SMAX - 1)]
        scores = (content + relative) * (HEAD ** -0.5)
        scores = jnp.where((distance >= 0)[None, :], scores, MASKED)
        weights = jax.nn.softmax(scores, axis=-1)
        return jnp.einsum('hs,shd->hd', weights, v_seq.astype(jnp.float32)).astype(jnp.bfloat16)

    context = lax.map(attend_one, (q_content, q_position, k_updated, v_updated, lengths))
    attn_out = jnp.dot(context.reshape(BATCH, HEADS * HEAD), w_out.reshape(HEADS * HEAD, D), preferred_element_type=jnp.float32)
    resid_mid = (hidden.astype(jnp.float32) + attn_out).astype(jnp.bfloat16)
    normed_mlp = rms_norm(resid_mid, g_mlp)
    up_proj = jnp.dot(normed_mlp, w_up, preferred_element_type=jnp.float32)
    activated = jax.nn.gelu(up_proj, approximate=True).astype(jnp.bfloat16)
    down_proj = jnp.dot(activated, w_down, preferred_element_type=jnp.float32)
    hidden_out = (resid_mid.astype(jnp.float32) + down_proj).astype(jnp.bfloat16)
    return hidden_out
```

```python
import functools

import jax
import jax.numpy as jnp
from jax import lax
from jax.experimental import pallas as pl
from jax.experimental.pallas import tpu as pltpu
from jax.sharding import PartitionSpec as P

EPS = 1e-6
MASKED = -1e30
MESH = pl.DeviceIdType.MESH
F32 = jnp.float32
BF16 = jnp.bfloat16
VMEM = pltpu.VMEM
NT = (((1,), (1,)), ((), ()))

BATCH, HEADS, HEAD, BLK, D = 16, 6, 128, 2048, 1536
TILES = BLK // 128
GROUPS, PER = 4, 4
GROWS = HEADS * PER
ROWS = GROUPS * GROWS
RING = 10
HID = 768


def rms_norm(wide, gain):
    mean_sq = jnp.mean(wide * wide, axis=-1, keepdims=True)
    return (wide * lax.rsqrt(mean_sq + EPS) * gain).astype(BF16)


def row_lengths(len_ref, group):
    seq = lax.rem(lax.broadcasted_iota(jnp.int32, (GROWS, 128), 0), PER)
    out = jnp.full((GROWS, 128), len_ref[PER * group], jnp.int32)
    for i in range(1, PER):
        out = jnp.where(seq == i, len_ref[PER * group + i], out)
    return out


def front_kernel(len_ref, x_ref, g_ref, u_ref, wb_ref, wq_hbm, wk_hbm, wv_hbm, rel_hbm,
                 qr_ref, rolled_ref, aux_ref, wq, wk, wv, rel, qf, raw, sems):
    copies = {}
    for h in range(HEADS):
        for j, (src, dst) in enumerate(((wq_hbm, wq), (rel_hbm, rel), (wk_hbm, wk), (wv_hbm, wv))):
            copies[j, h] = pltpu.make_async_copy(src.at[h], dst.at[h], sems.at[j, h])
    for j in range(4):
        for h in range(HEADS):
            copies[j, h].start()
    normed = rms_norm(x_ref[...].astype(F32), g_ref[...].astype(F32))
    qf[...] = jnp.zeros_like(qf)
    q_content = []
    for h in range(HEADS):
        copies[0, h].wait()
        q = jnp.dot(normed, wq[h], preferred_element_type=F32).astype(BF16).astype(F32)
        qc = (q + u_ref[h : h + 1, :].astype(F32)).astype(BF16).astype(F32)
        qp = (q + wb_ref[h : h + 1, :].astype(F32)).astype(BF16)
        q_content.append(qc)
        for s in range(GROUPS):
            row = s * GROWS + h * PER
            qf[row : row + PER, h * 128 : h * 128 + 128] = qc[s * PER : s * PER + PER, :]
        copies[1, h].wait()
        by_dist = lax.dot_general(qp, rel[h], NT, preferred_element_type=F32)
        for c in range(TILES):
            for s in range(GROUPS):
                row = s * GROWS + h * PER
                raw[c, row : row + PER, :] = by_dist[s * PER : s * PER + PER, c * 128 : c * 128 + 128]
    qr_ref[...] = qf[...].astype(BF16)
    lane = lax.broadcasted_iota(jnp.int32, (GROWS, 128), 1)
    for s in range(GROUPS):
        n = row_lengths(len_ref, s)
        r = lax.rem(n, BLK)
        big, small = lax.div(r, 128), lax.rem(r, 128)
        aux_ref[2, s * GROWS : s * GROWS + GROWS, :] = n.astype(F32)
        for t in range(GROWS // 8):
            sl = slice(8 * t, 8 * t + 8)
            row = s * GROWS + 8 * t
            idx = lax.rem(small[sl] - lane[sl] + 128, 128)
            tiles = [jnp.take_along_axis(raw[(TILES - c) % TILES, row : row + 8, :], idx, axis=1) for c in range(TILES)]
            for k in range(4):
                bit = lax.rem(lax.div(big[sl], 1 << k), 2) == 1
                tiles = [jnp.where(bit, tiles[(c - (1 << k)) % TILES], tiles[c]) for c in range(TILES)]
            low = lane[sl] <= small[sl]
            for c in range(TILES):
                rolled_ref[c, row : row + 8, :] = jnp.where(low, tiles[c], tiles[(c + 1) % TILES])
    for h in range(HEADS):
        copies[2, h].wait()
        kn = jnp.dot(normed, wk[h], preferred_element_type=F32).astype(BF16).astype(F32)
        copies[3, h].wait()
        vn = jnp.dot(normed, wv[h], preferred_element_type=F32).astype(BF16).astype(F32)
        sn = jnp.broadcast_to(jnp.sum(q_content[h] * kn, axis=1, keepdims=True), (BATCH, 128))
        for s in range(GROUPS):
            row = s * GROWS + h * PER
            aux_ref[0, row : row + PER, :] = sn[s * PER : s * PER + PER, :]
            aux_ref[1, row : row + PER, :] = vn[s * PER : s * PER + PER, :]


def main_kernel(k_hbm, v_hbm, qr_ref, rolled, aux, x_ref, g_ref, wo_hbm, wu_hbm, wd_hbm, out_ref,
                ring, wo, wu, wd, acc, score, from_pair, to_far, from_far, stat_out, stat_in, ctx, ctx_out, ctx_in,
                part_out, part_in, x1_ref, mlp_out, mlp_in, fin_out, fin_in,
                ring_sem, w_sem, pair_s, pair_r, far_s, far_r, stat_s, stat_r, ctx_s, ctx_r,
                part_s, part_r, mlp_s, mlp_r, fin_s, fin_r):
    tp, sp = lax.axis_index("tp"), lax.axis_index("sp")
    me = tp * 4 + sp
    odd = lax.rem(sp, 2)
    pair = sp + 1 - 2 * odd

    def load(step, slot):
        @pl.when(step < BATCH)
        def _():
            pltpu.make_async_copy(k_hbm.at[step], ring.at[slot], ring_sem.at[slot]).start()

        @pl.when(jnp.logical_and(step >= BATCH, step < 2 * BATCH))
        def _():
            pltpu.make_async_copy(v_hbm.at[step - BATCH], ring.at[slot], ring_sem.at[slot]).start()

    for i in range(RING):
        pltpu.make_async_copy(k_hbm.at[i], ring.at[i], ring_sem.at[i]).start()

    others = [(dt, ds) for dt in range(2) for ds in range(4) if (dt, ds) != (0, 0)]

    def peer(dt, ds):
        return lax.rem(tp + dt, 2), lax.rem(sp + ds, 4)

    def source(dt, ds):
        return lax.rem(tp + 2 - dt, 2), lax.rem(sp + 4 - ds, 4)

    barrier = pltpu.get_barrier_semaphore()
    for dt, ds in others:
        t, s = peer(dt, ds)
        pl.semaphore_signal(barrier, inc=1, device_id={"tp": t, "sp": s}, device_id_type=MESH)
    pl.semaphore_wait(barrier, 7)

    def remote(src, dst, send, recv, t, s):
        return pltpu.make_async_remote_copy(
            src_ref=src, dst_ref=dst, send_sem=send, recv_sem=recv, device_id={"tp": t, "sp": s}, device_id_type=MESH
        )

    def rows(g):
        return pl.ds(g * GROWS, GROWS)

    def pair_copy(g):
        return remote(rolled.at[:, rows(g), :], from_pair.at[:, rows(g), :], pair_s.at[g], pair_r.at[g], tp, pair)

    def far_copy(g):
        return remote(to_far.at[:, rows(g), :], from_far.at[:, rows(g), :], far_s.at[g], far_r.at[g], tp, 3 - sp)

    for g in range(GROUPS):
        pair_copy(g).start()

    lane = lax.broadcasted_iota(jnp.int32, (GROWS, 128), 1)
    row_id = lax.broadcasted_iota(jnp.int32, (128, 256), 0)
    row_seq = lax.div(row_id, GROWS) * PER + lax.rem(row_id, PER)
    acc[...] = jnp.zeros_like(acc)

    def k_step(b, _):
        slot = lax.rem(b, RING)
        pltpu.make_async_copy(k_hbm.at[b], ring.at[slot], ring_sem.at[slot]).wait()
        total = None
        for p in range(HEADS // 2):
            keys = jnp.concatenate([ring[slot, 2 * p], ring[slot, 2 * p + 1]], axis=1)
            query = jnp.where(row_seq == b, qr_ref[:, 256 * p : 256 * p + 256], jnp.zeros((), BF16))
            dots = lax.dot_general(keys, query, NT, preferred_element_type=F32)
            total = dots if total is None else total + dots
        acc[...] += total
        load(b + RING, slot)

        @pl.when(b == 2)
        def _():
            for g in range(GROUPS):
                pair_copy(g).wait()
                n = aux[2, g * GROWS : g * GROWS + GROWS, :].astype(jnp.int32)
                r = lax.rem(n, BLK)
                last = lax.div(n, BLK) == 3
                for c in range(TILES):
                    mine = jnp.logical_or(jnp.logical_and(last, lane + 128 * c <= r), odd == 0)
                    to_far[c, g * GROWS : g * GROWS + GROWS, :] = jnp.where(
                        mine, rolled[c, g * GROWS : g * GROWS + GROWS, :], from_pair[c, g * GROWS : g * GROWS + GROWS, :]
                    )

        @pl.when(b == 3)
        def _():
            for g in range(GROUPS):
                far_copy(g).start()

        return 0

    lax.fori_loop(0, BATCH, k_step, 0)

    weights = (
        pltpu.make_async_copy(wo_hbm, wo, w_sem.at[0]),
        pltpu.make_async_copy(wu_hbm.at[:, pl.ds(pl.multiple_of(sp * HID, 128), HID)], wu, w_sem.at[1]),
        pltpu.make_async_copy(wd_hbm.at[pl.ds(pl.multiple_of(sp * HID, 128), HID), :], wd, w_sem.at[2]),
    )
    for w in weights:
        w.start()
    for c in range(TILES):
        score[c] = jnp.transpose(acc[128 * c : 128 * c + 128, :])[:ROWS]

    def softmax(g):
        base = pl.multiple_of(g * GROWS, 8)
        sl = pl.ds(base, GROWS)
        far_copy(g).wait()
        n = aux[2, sl, :].astype(jnp.int32)
        new = aux[0, sl, :]
        r = lax.rem(n, BLK)
        block = lax.div(n, BLK) - sp
        here = n - sp * BLK
        top = jnp.full((GROWS, 128), MASKED, F32)
        for c in range(TILES):
            pos = lane + 128 * c
            owner = jnp.where(pos <= r, block, block - 1)
            rel = jnp.where(owner == sp, rolled[c, sl, :], jnp.where(owner == pair, from_pair[c, sl, :], from_far[c, sl, :]))
            content = jnp.where(pos == here, new, score[c, sl, :])
            sc = jnp.where(pos <= here, (content + rel) * (HEAD**-0.5), MASKED)
            score[c, sl, :] = sc
            top = jnp.maximum(top, sc)
        top = jnp.max(top, axis=1, keepdims=True)
        total = jnp.zeros((GROWS, 128), F32)
        at_new = jnp.zeros((GROWS, 128), F32)
        for c in range(TILES):
            pos = lane + 128 * c
            w = jnp.where(pos <= here, jnp.exp(score[c, sl, :] - top), 0.0)
            total = total + w
            at_new = at_new + jnp.where(pos == here, w.astype(BF16).astype(F32), 0.0)
            score[c, sl, :] = jnp.where(pos == here, 0.0, w)
        total = jnp.sum(total, axis=1, keepdims=True)
        at_new = jnp.sum(at_new, axis=1, keepdims=True)
        stat_out[sl, :] = jnp.where(lane < 64, top, total)
        ctx_out_scale = jnp.broadcast_to(at_new, (GROWS, 128))
        acc[sl, :] = ctx_out_scale

    def stat_copy(ds):
        t, s = peer(0, ds)
        return remote(stat_out, stat_in.at[ds - 1], stat_s.at[ds - 1], stat_r.at[ds - 1], t, s)

    head_row = lax.broadcasted_iota(jnp.int32, (HEADS, 128), 0)

    def v_step(b, _):
        g, i = lax.div(b, PER), lax.rem(b, PER)

        @pl.when(i == 0)
        def _():
            softmax(g)

        slot = lax.rem(b + BATCH, RING)
        pltpu.make_async_copy(v_hbm.at[b], ring.at[slot], ring_sem.at[slot]).wait()
        first = g * GROWS + i
        probs = jnp.concatenate([score[c, pl.ds(first, HEADS, stride=PER), :] for c in range(TILES)], axis=1).astype(BF16)
        out = jnp.zeros((HEADS, 128), F32)
        for h in range(HEADS):
            dots = jnp.dot(probs, ring[slot, h], preferred_element_type=F32)
            out = jnp.where(head_row == h, dots, out)
        ctx[pl.ds(first, HEADS, stride=PER), :] = out
        load(b + BATCH + RING, slot)

        @pl.when(b == BATCH - PER)
        def _():
            for ds in range(1, 4):
                stat_copy(ds).start()

        return 0

    lax.fori_loop(0, BATCH, v_step, 0)

    for ds in range(1, 4):
        stat_copy(ds).wait()
    mine = stat_out[...]
    top, total = mine[:, :1], mine[:, 64:65]
    all_top = top
    for ds in range(3):
        all_top = jnp.maximum(all_top, stat_in[ds, :, :1])
    all_total = total * jnp.exp(top - all_top)
    for ds in range(3):
        all_total = all_total + stat_in[ds, :, 64:65] * jnp.exp(stat_in[ds, :, :1] - all_top)
    scale = jnp.exp(top - all_top) / all_total
    scaled = (ctx[...] + acc[:ROWS, :] * aux[1]) * scale
    for g in range(GROUPS):
        ctx_out[g] = scaled[g * GROWS : g * GROWS + GROWS, :]

    def ctx_copy(ds):
        t, s = peer(0, ds)
        return remote(ctx_out.at[s], ctx_in.at[ds], ctx_s.at[ds - 1], ctx_r.at[ds - 1], t, s)

    for ds in range(1, 4):
        ctx_copy(ds).start()
    for w in weights:
        w.wait()
    ctx_in[0] = ctx_out[sp]
    for ds in range(1, 4):
        ctx_copy(ds).wait()
    whole = ((ctx_in[0] + ctx_in[1]) + (ctx_in[2] + ctx_in[3])).astype(BF16).astype(F32)
    lhs = jnp.concatenate([whole[h * PER : h * PER + PER, :] for h in range(HEADS)], axis=1).astype(BF16)
    part_out[...] = jnp.dot(lhs, wo[...], preferred_element_type=F32)

    def part_copy(j, sending):
        t, s = peer(*others[j])
        ft, fs = source(*others[j])
        slot = me if sending else ft * 4 + fs
        return remote(part_out, part_in.at[slot], part_s.at[j], part_r.at[j], t, s)

    for j in range(7):
        part_copy(j, True).start()
    part_in[me] = part_out[...]
    for j in range(7):
        part_copy(j, True).wait_send()
        part_copy(j, False).wait_recv()
    attn = jnp.concatenate([part_in[s] + part_in[4 + s] for s in range(GROUPS)], axis=0)
    x1 = (x_ref[...].astype(F32) + attn).astype(BF16).astype(F32)
    for k in range(8):
        x1_ref[k] = x1[2 * k : 2 * k + 2, :]
    normed = rms_norm(x1, g_ref[...].astype(F32))
    up = jnp.dot(normed, wu[...], preferred_element_type=F32)
    act = jax.nn.gelu(up, approximate=True).astype(BF16)
    down = jnp.dot(act, wd[...], preferred_element_type=F32)
    for k in range(8):
        mlp_out[k] = down[2 * k : 2 * k + 2, :]

    def mlp_copy(j, sending):
        t, s = peer(*others[j])
        ft, fs = source(*others[j])
        slot = me if sending else ft * 4 + fs
        return remote(mlp_out.at[t * 4 + s], mlp_in.at[slot], mlp_s.at[j], mlp_r.at[j], t, s)

    for j in range(7):
        mlp_copy(j, True).start()
    mlp_in[me] = mlp_out[me]
    for j in range(7):
        mlp_copy(j, True).wait_send()
        mlp_copy(j, False).wait_recv()
    tot = mlp_in[0]
    for k in range(1, 8):
        tot = tot + mlp_in[k]
    fin_out[...] = (x1_ref[me] + tot).astype(BF16).astype(F32)

    def fin_copy(j, sending):
        t, s = peer(*others[j])
        ft, fs = source(*others[j])
        slot = me if sending else ft * 4 + fs
        return remote(fin_out, fin_in.at[slot], fin_s.at[j], fin_r.at[j], t, s)

    for j in range(7):
        fin_copy(j, True).start()
    fin_in[me] = fin_out[...]
    for j in range(7):
        fin_copy(j, True).wait_send()
        fin_copy(j, False).wait_recv()
    out_ref[...] = jnp.concatenate([fin_in[k] for k in range(8)], axis=0).astype(BF16)


def solution(mesh):
    spec_rows = P('dp', None)
    spec_cache = P('dp', 'sp', 'tp', None)
    in_specs = (spec_rows, spec_cache, spec_cache, P('dp'), P('sp', 'tp', None), P('tp', None), P('tp', None), P(None), P(None, 'tp', None), P(None, 'tp', None), P(None, 'tp', None), P('tp', None, None), P(None), P(None, 'tp'), P('tp', None))
    out_specs = spec_rows
    vm = pl.BlockSpec(memory_space=VMEM)
    hbm = pl.BlockSpec(memory_space=pl.ANY)
    smem = pl.BlockSpec(memory_space=pltpu.SMEM)
    dma = pltpu.SemaphoreType.DMA

    def layer_step(hidden, k_cache, v_cache, lengths, rel_table, u_bias, w_bias, g_attn, w_query, w_key, w_value, w_out, g_mlp, w_up, w_down):
        heads_first = lambda w: jnp.transpose(w, (1, 0, 2))
        qr, rolled, aux = pl.pallas_call(
            front_kernel,
            out_shape=(
                jax.ShapeDtypeStruct((128, HEADS * HEAD), BF16),
                jax.ShapeDtypeStruct((TILES, ROWS, 128), F32),
                jax.ShapeDtypeStruct((3, ROWS, 128), F32),
            ),
            in_specs=[smem, vm, vm, vm, vm, hbm, hbm, hbm, hbm],
            out_specs=(vm, vm, vm),
            scratch_shapes=[
                VMEM((HEADS, D, HEAD), BF16), VMEM((HEADS, D, HEAD), BF16), VMEM((HEADS, D, HEAD), BF16),
                VMEM((HEADS, BLK, HEAD), BF16), VMEM((128, HEADS * HEAD), F32), VMEM((TILES, ROWS, 128), F32),
                dma((4, HEADS)),
            ],
            compiler_params=pltpu.CompilerParams(vmem_limit_bytes=60 * 2**20),
            name="front",
        )(lengths, hidden, g_attn.reshape(1, D), u_bias, w_bias, heads_first(w_query), heads_first(w_key), heads_first(w_value), heads_first(rel_table))
        return pl.pallas_call(
            main_kernel,
            out_shape=jax.ShapeDtypeStruct((BATCH, D), BF16),
            in_specs=[hbm, hbm, vm, vm, vm, vm, vm, hbm, hbm, hbm],
            out_specs=vm,
            scratch_shapes=[
                VMEM((RING, HEADS, BLK, HEAD), BF16),
                VMEM((HEADS * HEAD, D), BF16), VMEM((D, HID), BF16), VMEM((HID, D), BF16),
                VMEM((BLK, 128), F32), VMEM((TILES, ROWS, 128), F32),
                VMEM((TILES, ROWS, 128), F32), VMEM((TILES, ROWS, 128), F32), VMEM((TILES, ROWS, 128), F32),
                VMEM((ROWS, 128), F32), VMEM((3, ROWS, 128), F32), VMEM((ROWS, 128), F32),
                VMEM((GROUPS, GROWS, 128), F32), VMEM((4, GROWS, 128), F32),
                VMEM((PER, D), F32), VMEM((8, PER, D), F32), VMEM((8, 2, D), F32),
                VMEM((8, 2, D), F32), VMEM((8, 2, D), F32), VMEM((2, D), F32), VMEM((8, 2, D), F32),
                dma((RING,)), dma((3,)), dma((4,)), dma((4,)), dma((4,)), dma((4,)), dma((3,)), dma((3,)), dma((3,)), dma((3,)),
                dma((7,)), dma((7,)), dma((7,)), dma((7,)), dma((7,)), dma((7,)),
            ],
            compiler_params=pltpu.CompilerParams(vmem_limit_bytes=60 * 2**20, collective_id=0, has_side_effects=True),
            name="main",
        )(
            jnp.transpose(k_cache, (0, 2, 1, 3)), jnp.transpose(v_cache, (0, 2, 1, 3)), qr, rolled, aux,
            hidden, g_mlp.reshape(1, D), w_out.reshape(HEADS * HEAD, D), w_up, w_down,
        )

    return jax.shard_map(layer_step, mesh=mesh, in_specs=in_specs, out_specs=out_specs, check_vma=False)
```

```python
import functools

import jax
import jax.numpy as jnp
from jax import lax
from jax.experimental import pallas as pl
from jax.experimental.pallas import tpu as pltpu
from jax.sharding import PartitionSpec as P

EPS = 1e-6
MASKED = -1e30
MESH = pl.DeviceIdType.MESH
F32 = jnp.float32
BF16 = jnp.bfloat16
VMEM = pltpu.VMEM
NT = (((1,), (1,)), ((), ()))

BATCH, HEADS, HEAD, BLK, D = 16, 6, 128, 2048, 1536
TILES = BLK // 128
GROUPS, PER = 4, 4
GROWS = HEADS * PER
ROWS = GROUPS * GROWS
RING = 9
HID = 768


def rms_norm(wide, gain):
    mean_sq = jnp.mean(wide * wide, axis=-1, keepdims=True)
    return (wide * lax.rsqrt(mean_sq + EPS) * gain).astype(BF16)


def fused_kernel(len_ref, x_hbm, g1_hbm, g2_hbm, u_hbm, wb_hbm, wq_hbm, wk_hbm, wv_hbm, rel_hbm, k_hbm, v_hbm, wo_hbm, wu_hbm, wd_hbm,
                 out_ref,
                 xb, g1, g2, ub, wbb, wq, wk, wv, rel, qf, qc_ref, raw, new_score, new_value, new_prob,
                 ring, wo, wu, wd, score, rolled, from_pair, to_far, from_far, probs, stat_out, stat_in, ctx, ctx_in,
                 part_out, part_in, x1_ref, mlp_in,
                 small_sem, in_sem, ring_sem, w_sem, pair_s, pair_r, far_s, far_r, stat_s, stat_r, ctx_s, ctx_r,
                 part_s, part_r, mlp_s, mlp_r):
    tp, sp = lax.axis_index("tp"), lax.axis_index("sp")
    me = tp * 4 + sp
    odd = lax.rem(sp, 2)
    pair = sp + 1 - 2 * odd

    small = [pltpu.make_async_copy(a, b, small_sem.at[i]) for i, (a, b) in enumerate(
        ((x_hbm, xb), (g1_hbm, g1), (g2_hbm, g2), (u_hbm, ub), (wb_hbm, wbb)))]

    def head_copy(j, h):
        a, b = ((wq_hbm, wq), (rel_hbm, rel), (wk_hbm, wk), (wv_hbm, wv))[j]
        return pltpu.make_async_copy(a.at[h], b.at[h], in_sem.at[j, h])

    weights = (
        pltpu.make_async_copy(wo_hbm, wo, w_sem.at[0]),
        pltpu.make_async_copy(wu_hbm.at[:, pl.ds(pl.multiple_of(sp * HID, 128), HID)], wu, w_sem.at[1]),
        pltpu.make_async_copy(wd_hbm.at[pl.ds(pl.multiple_of(sp * HID, 128), HID), :], wd, w_sem.at[2]),
    )

    def load(step, slot):
        @pl.when(step < BATCH)
        def _():
            pltpu.make_async_copy(k_hbm.at[step], ring.at[slot], ring_sem.at[slot]).start()

        @pl.when(jnp.logical_and(step >= BATCH, step < 2 * BATCH))
        def _():
            pltpu.make_async_copy(v_hbm.at[step - BATCH], ring.at[slot], ring_sem.at[slot]).start()

    for c in small:
        c.start()
    for j in range(2):
        for h in range(HEADS):
            head_copy(j, h).start()
    for i in range(RING):
        pltpu.make_async_copy(k_hbm.at[i], ring.at[i], ring_sem.at[i]).start()

    others = [(dt, ds) for dt in range(2) for ds in range(4) if (dt, ds) != (0, 0)]

    def peer(dt, ds):
        return lax.rem(tp + dt, 2), lax.rem(sp + ds, 4)

    def source(dt, ds):
        return lax.rem(tp + 2 - dt, 2), lax.rem(sp + 4 - ds, 4)

    barrier = pltpu.get_barrier_semaphore()
    for dt, ds in others:
        t, s = peer(dt, ds)
        pl.semaphore_signal(barrier, inc=1, device_id={"tp": t, "sp": s}, device_id_type=MESH)

    def remote(src, dst, send, recv, t, s):
        return pltpu.make_async_remote_copy(
            src_ref=src, dst_ref=dst, send_sem=send, recv_sem=recv, device_id={"tp": t, "sp": s}, device_id_type=MESH
        )

    def rows(g):
        return pl.ds(pl.multiple_of(g * GROWS, 8), GROWS)

    def pair_copy(g):
        return remote(rolled.at[:, rows(g), :], from_pair.at[:, rows(g), :], pair_s.at[g], pair_r.at[g], tp, pair)

    def far_copy(g):
        return remote(to_far.at[:, rows(g), :], from_far.at[:, rows(g), :], far_s.at[g], far_r.at[g], tp, 3 - sp)

    def stat_copy(g, ds):
        t, s = peer(0, ds)
        return remote(stat_out.at[rows(g), :], stat_in.at[ds - 1, rows(g), :], stat_s.at[g, ds - 1], stat_r.at[g, ds - 1], t, s)

    def ctx_copy(g, ds, sending):
        t, s = peer(0, ds)
        _, fs = source(0, ds)
        slot = sp if sending else fs
        return remote(ctx_in.at[slot, rows(g), :], ctx_in.at[slot, rows(g), :], ctx_s.at[g, ds - 1], ctx_r.at[g, ds - 1], t, s)

    def part_copy(g):
        return remote(part_out.at[g], part_in.at[g], part_s.at[g], part_r.at[g], 1 - tp, sp)

    def mlp_copy(g, j, sending):
        t, s = peer(*others[j])
        ft, fs = source(*others[j])
        slot = me if sending else ft * 4 + fs
        return remote(mlp_in.at[g, slot], mlp_in.at[g, slot], mlp_s.at[g, j], mlp_r.at[g, j], t, s)

    for c in small:
        c.wait()
    x = xb[...].astype(F32)
    for g in range(GROUPS):
        x1_ref[g] = x[PER * g : PER * g + PER, :]
    normed = rms_norm(x, g1[...].astype(F32).reshape(1, D))
    qf[...] = jnp.zeros_like(qf)
    for h in range(HEADS):
        head_copy(0, h).wait()
        q = jnp.dot(normed, wq[h], preferred_element_type=F32).astype(BF16).astype(F32)
        qc = (q + ub[h : h + 1, :].astype(F32)).astype(BF16).astype(F32)
        qp = (q + wbb[h : h + 1, :].astype(F32)).astype(BF16)
        qc_ref[h] = qc
        qf[h, pl.ds(h, BATCH, stride=8), :] = qc
        head_copy(1, h).wait()
        by_dist = lax.dot_general(qp, rel[h], NT, preferred_element_type=F32)
        for c in range(TILES):
            for s in range(GROUPS):
                row = s * GROWS + h * PER
                raw[c, row : row + PER, :] = by_dist[s * PER : s * PER + PER, c * 128 : c * 128 + 128]

    def lengths_of(group, count):
        seq = lax.rem(lax.broadcasted_iota(jnp.int32, (count, 128), 0), PER)
        out = jnp.zeros((count, 128), jnp.int32) + len_ref[PER * group]
        for i in range(1, PER):
            out = jnp.where(seq == i, len_ref[PER * group + i], out)
        return out

    lane8 = lax.broadcasted_iota(jnp.int32, (8, 128), 1)

    def roll(piece):
        r = lax.rem(lengths_of(lax.div(piece, GROWS // 8), 8), BLK)
        big, small_r = lax.div(r, 128), lax.rem(r, 128)
        sl = pl.ds(pl.multiple_of(piece * 8, 8), 8)
        idx = lax.rem(small_r - lane8 + 128, 128)
        tiles = [jnp.take_along_axis(raw[(TILES - c) % TILES, sl, :], idx, axis=1) for c in range(TILES)]
        for k in range(4):
            bit = lax.rem(lax.div(big, 1 << k), 2) == 1
            tiles = [jnp.where(bit, tiles[(c - (1 << k)) % TILES], tiles[c]) for c in range(TILES)]
        low = lane8 <= small_r
        for c in range(TILES):
            rolled[c, sl, :] = jnp.where(low, tiles[c], tiles[(c + 1) % TILES])

    def content(b):
        slot = lax.rem(b, RING)
        pltpu.make_async_copy(k_hbm.at[b], ring.at[slot], ring_sem.at[slot]).wait()
        sl = pl.ds(pl.multiple_of(b * 8, 8), 8)
        total = None
        for p in range(HEADS // 2):
            keys = jnp.concatenate([ring[slot, 2 * p], ring[slot, 2 * p + 1]], axis=1)
            query = jnp.concatenate([qf[2 * p, sl, :], qf[2 * p + 1, sl, :]], axis=1).astype(BF16)
            dots = lax.dot_general(query, keys, NT, preferred_element_type=F32)
            total = dots if total is None else total + dots
        first = lax.div(b, PER) * GROWS + lax.rem(b, PER)
        for c in range(TILES):
            score[c, pl.ds(first, HEADS, stride=PER), :] = total[:HEADS, c * 128 : c * 128 + 128]
        return slot

    lane24 = lax.broadcasted_iota(jnp.int32, (GROWS, 128), 1)

    def merge(g):
        pair_copy(g).wait()
        n = lengths_of(g, GROWS)
        r = lax.rem(n, BLK)
        last = lax.div(n, BLK) == 3
        for c in range(TILES):
            mine = jnp.logical_or(jnp.logical_and(last, lane24 + 128 * c <= r), odd == 0)
            to_far[c, rows(g), :] = jnp.where(mine, rolled[c, rows(g), :], from_pair[c, rows(g), :])

    def k_tail(b, slot):
        load(b + RING, slot)
        g, i = lax.div(b, 3), lax.rem(b, 3)

        @pl.when(jnp.logical_and(i == 2, g < GROUPS))
        def _():
            pair_copy(g).start()

        @pl.when(jnp.logical_and(i == 2, g >= 1))
        def _():
            merge(g - 1)

        @pl.when(jnp.logical_and(i == 0, g >= 2))
        def _():
            far_copy(g - 2).start()

    pl.semaphore_wait(barrier, 7)

    def k_early(b, _):
        slot = content(b)
        roll(b)
        k_tail(b, slot)

        @pl.when(b == 2)
        def _():
            for j in (2, 3):
                for h in range(HEADS):
                    head_copy(j, h).start()

        @pl.when(b == 8)
        def _():
            for w in weights:
                w.start()

        return 0

    def k_late(b, _):
        slot = content(b)
        k_tail(b, slot)
        return 0

    lax.fori_loop(0, 12, k_early, 0)
    for h in range(HEADS):
        head_copy(2, h).wait()
        kn = jnp.dot(normed, wk[h], preferred_element_type=F32).astype(BF16).astype(F32)
        head_copy(3, h).wait()
        vn = jnp.dot(normed, wv[h], preferred_element_type=F32).astype(BF16).astype(F32)
        sn = jnp.broadcast_to(jnp.sum(qc_ref[h] * kn, axis=1, keepdims=True), (BATCH, 128))
        for s in range(GROUPS):
            row = s * GROWS + h * PER
            new_score[row : row + PER, :] = sn[s * PER : s * PER + PER, :]
            new_value[row : row + PER, :] = vn[s * PER : s * PER + PER, :]
    lax.fori_loop(12, BATCH, k_late, 0)

    lane6 = lax.broadcasted_iota(jnp.int32, (HEADS, 128), 1)
    head_row = lax.broadcasted_iota(jnp.int32, (HEADS, 128), 0)

    def softmax(b):
        sl = pl.ds(lax.div(b, PER) * GROWS + lax.rem(b, PER), HEADS, stride=PER)
        n = len_ref[b]
        r = lax.rem(n, BLK)
        block = lax.div(n, BLK)
        here = n - sp * BLK
        new = new_score[sl, :]
        own_a, pair_a = block - sp == sp, block - sp == pair
        own_b, pair_b = block - sp - 1 == sp, block - sp - 1 == pair
        sc = []
        for c in range(TILES):
            pos = lane6 + 128 * c
            own, near, far = rolled[c, sl, :], from_pair[c, sl, :], from_far[c, sl, :]
            rel_a = jnp.where(own_a, own, jnp.where(pair_a, near, far))
            rel_b = jnp.where(own_b, own, jnp.where(pair_b, near, far))
            rel_c = jnp.where(pos <= r, rel_a, rel_b)
            con = jnp.where(pos == here, new, score[c, sl, :])
            sc.append(jnp.where(pos <= here, (con + rel_c) * (HEAD**-0.5), MASKED))
        top = functools.reduce(jnp.maximum, sc)
        top = jnp.max(top, axis=1, keepdims=True)
        total = jnp.zeros((HEADS, 128), F32)
        at_new = jnp.zeros((HEADS, 128), F32)
        slot = lax.rem(b, 3)
        for c in range(TILES):
            pos = lane6 + 128 * c
            w = jnp.where(pos <= here, jnp.exp(sc[c] - top), 0.0)
            total = total + w
            at_new = at_new + jnp.where(pos == here, w.astype(BF16).astype(F32), 0.0)
            probs[slot, :, c * 128 : c * 128 + 128] = jnp.where(pos == here, 0.0, w)
        total = jnp.sum(total, axis=1, keepdims=True)
        at_new = jnp.sum(at_new, axis=1, keepdims=True)
        stat_out[sl, :] = jnp.where(lane6 < 64, top, total)
        new_prob[sl, :] = jnp.broadcast_to(at_new, (HEADS, 128))

    def attend(b):
        slot = lax.rem(b + BATCH, RING)
        pltpu.make_async_copy(v_hbm.at[b], ring.at[slot], ring_sem.at[slot]).wait()
        pb = probs[lax.rem(b, 3)].astype(BF16)
        out = jnp.zeros((HEADS, 128), F32)
        for p in range(HEADS // 2):
            values = jnp.concatenate([ring[slot, 2 * p], ring[slot, 2 * p + 1]], axis=1)
            dots = jnp.dot(pb, values, preferred_element_type=F32)
            out = jnp.where(head_row == 2 * p, dots[:, :128], jnp.where(head_row == 2 * p + 1, dots[:, 128:], out))
        ctx[pl.ds(lax.div(b, PER) * GROWS + lax.rem(b, PER), HEADS, stride=PER), :] = out
        return slot

    def send_stats(g):
        for ds in range(1, 4):
            stat_copy(g, ds).start()

    def send_ctx(g):
        for ds in range(1, 4):
            stat_copy(g, ds).wait()
        mine = stat_out[rows(g), :]
        top, total = mine[:, :1], mine[:, 64:65]
        all_top = top
        for ds in range(3):
            all_top = jnp.maximum(all_top, stat_in[ds, rows(g), :][:, :1])
        all_total = total * jnp.exp(top - all_top)
        for ds in range(3):
            got = stat_in[ds, rows(g), :]
            all_total = all_total + got[:, 64:65] * jnp.exp(got[:, :1] - all_top)
        scale = jnp.exp(top - all_top) / all_total
        ctx_in[sp, rows(g), :] = (ctx[rows(g), :] + new_prob[rows(g), :] * new_value[rows(g), :]) * scale
        for ds in range(1, 4):
            ctx_copy(g, ds, True).start()

    def project(g):
        for ds in range(1, 4):
            ctx_copy(g, ds, True).wait_send()
            ctx_copy(g, ds, False).wait_recv()
        whole = (ctx_in[0, rows(g), :] + ctx_in[1, rows(g), :]) + (ctx_in[2, rows(g), :] + ctx_in[3, rows(g), :])
        lhs = jnp.concatenate([whole[h * PER : h * PER + PER, :] for h in range(HEADS)], axis=1).astype(BF16)
        part_out[g] = jnp.dot(lhs, wo[...], preferred_element_type=F32)
        part_copy(g).start()

    def mlp(g):
        part_copy(g).wait()
        x1 = (x1_ref[g] + (part_out[g] + part_in[g])).astype(BF16).astype(F32)
        x1_ref[g] = x1
        up = jnp.dot(rms_norm(x1, g2[...].astype(F32).reshape(1, D)), wu[...], preferred_element_type=F32)
        act = jax.nn.gelu(up, approximate=True).astype(BF16)
        mlp_in[g, me] = jnp.dot(act, wd[...], preferred_element_type=F32)
        for j in range(7):
            mlp_copy(g, j, True).start()

    def finish(g):
        for j in range(7):
            mlp_copy(g, j, True).wait_send()
            mlp_copy(g, j, False).wait_recv()
        tot = mlp_in[g, 0]
        for k in range(1, 8):
            tot = tot + mlp_in[g, k]
        return x1_ref[g] + tot

    far_copy(0).wait()
    softmax(0)
    softmax(1)

    def v_step(b, _):
        g, i = lax.div(b, PER), lax.rem(b, PER)

        @pl.when(jnp.logical_and(i == 2, g < GROUPS - 1))
        def _():
            far_copy(g + 1).wait()

        slot = attend(b)
        softmax(b + 2)
        load(b + BATCH + RING, slot)

        @pl.when(b == 3)
        def _():
            for w in weights:
                w.wait()

        @pl.when(i == 1)
        def _():
            send_stats(g)

        @pl.when(i == 3)
        def _():
            send_ctx(g)

        @pl.when(jnp.logical_and(i == 2, g >= 1))
        def _():
            project(g - 1)

        @pl.when(jnp.logical_and(i == 1, g >= 2))
        def _():
            mlp(g - 2)

        return 0

    lax.fori_loop(0, BATCH - 2, v_step, 0)
    attend(jnp.int32(BATCH - 2))
    project(GROUPS - 2)
    attend(jnp.int32(BATCH - 1))
    send_ctx(GROUPS - 1)
    mlp(GROUPS - 2)
    project(GROUPS - 1)
    done = [finish(0), finish(1)]
    mlp(GROUPS - 1)
    done = done + [finish(2), finish(3)]
    out_ref[...] = jnp.concatenate(done, axis=0).astype(BF16)


def solution(mesh):
    spec_rows = P('dp', None)
    spec_cache = P('dp', 'sp', 'tp', None)
    in_specs = (spec_rows, spec_cache, spec_cache, P('dp'), P('sp', 'tp', None), P('tp', None), P('tp', None), P(None), P(None, 'tp', None), P(None, 'tp', None), P(None, 'tp', None), P('tp', None, None), P(None), P(None, 'tp'), P('tp', None))
    out_specs = spec_rows
    vm = pl.BlockSpec(memory_space=VMEM)
    hbm = pl.BlockSpec(memory_space=pl.ANY)
    smem = pl.BlockSpec(memory_space=pltpu.SMEM)
    dma = pltpu.SemaphoreType.DMA
    head_weight = VMEM((HEADS, D, HEAD), BF16)
    tiles = VMEM((TILES, ROWS, 128), F32)
    by_row = VMEM((ROWS, 128), F32)

    def layer_step(hidden, k_cache, v_cache, lengths, rel_table, u_bias, w_bias, g_attn, w_query, w_key, w_value, w_out, g_mlp, w_up, w_down):
        heads_first = lambda w: jnp.transpose(w, (1, 0, 2))
        return pl.pallas_call(
            fused_kernel,
            out_shape=jax.ShapeDtypeStruct((BATCH, D), BF16),
            in_specs=[smem] + [hbm] * 14,
            out_specs=vm,
            scratch_shapes=[
                VMEM((BATCH, D), BF16), VMEM((D,), BF16), VMEM((D,), BF16), VMEM((HEADS, HEAD), BF16), VMEM((HEADS, HEAD), BF16),
                head_weight, head_weight, head_weight, VMEM((HEADS, BLK, HEAD), BF16),
                VMEM((HEADS, 128, 128), F32), VMEM((HEADS, BATCH, 128), F32), tiles, by_row, by_row, by_row,
                VMEM((RING, HEADS, BLK, HEAD), BF16), VMEM((HEADS * HEAD, D), BF16), VMEM((D, HID), BF16), VMEM((HID, D), BF16),
                tiles, tiles, tiles, tiles, tiles, VMEM((3, HEADS, BLK), F32),
                by_row, VMEM((3, ROWS, 128), F32), by_row, VMEM((4, ROWS, 128), F32),
                VMEM((GROUPS, PER, D), F32), VMEM((GROUPS, PER, D), F32), VMEM((GROUPS, PER, D), F32), VMEM((GROUPS, 8, PER, D), F32),
                dma((5,)), dma((4, HEADS)), dma((RING,)), dma((3,)), dma((4,)), dma((4,)), dma((4,)), dma((4,)),
                dma((4, 3)), dma((4, 3)), dma((4, 3)), dma((4, 3)), dma((4,)), dma((4,)), dma((4, 7)), dma((4, 7)),
            ],
            compiler_params=pltpu.CompilerParams(vmem_limit_bytes=63 * 2**20, collective_id=0, has_side_effects=True),
            name="layer",
        )(
            lengths, hidden, g_attn, g_mlp, u_bias, w_bias,
            heads_first(w_query), heads_first(w_key), heads_first(w_value), heads_first(rel_table),
            jnp.transpose(k_cache, (0, 2, 1, 3)), jnp.transpose(v_cache, (0, 2, 1, 3)),
            w_out.reshape(HEADS * HEAD, D), w_up, w_down,
        )

    return jax.shard_map(layer_step, mesh=mesh, in_specs=in_specs, out_specs=out_specs, check_vma=False)
```

```python
import functools

import jax
import jax.numpy as jnp
from jax import lax
from jax.experimental import pallas as pl
from jax.experimental.pallas import tpu as pltpu
from jax.sharding import PartitionSpec as P

EPS = 1e-6
MASKED = -1e30
MESH = pl.DeviceIdType.MESH
F32 = jnp.float32
BF16 = jnp.bfloat16
VMEM = pltpu.VMEM
NT = (((1,), (1,)), ((), ()))

BATCH, HEADS, HEAD, BLK, D = 16, 6, 128, 2048, 1536
TILES = BLK // 128
GROUPS, PER = 4, 4
GROWS = HEADS * PER
ROWS = GROUPS * GROWS
RING = 8
FIRST = 3
HID = 768


def rms_norm(wide, gain):
    mean_sq = jnp.mean(wide * wide, axis=-1, keepdims=True)
    return (wide * lax.rsqrt(mean_sq + EPS) * gain).astype(BF16)


def fused_kernel(len_ref, x_hbm, g1_hbm, g2_hbm, u_hbm, wb_hbm, wq_hbm, wk_hbm, wv_hbm, rel_hbm, k_hbm, v_hbm, wo_hbm, wu_hbm, wd_hbm,
                 out_ref,
                 xb, g1, g2, ub, wbb, wq, wk, wv, rel, qf, qc_ref, raw, new_score, new_value, new_prob,
                 ring, wo, wu, wd, score, rolled, from_pair, to_far, from_far, probs, stat_out, stat_in, ctx, ctx_in,
                 part_out, part_in, x1_ref, mlp_in,
                 small_sem, in_sem, ring_sem, w_sem, pair_s, pair_r, far_s, far_r, stat_s, stat_r, ctx_s, ctx_r,
                 part_s, part_r, mlp_s, mlp_r):
    tp, sp = lax.axis_index("tp"), lax.axis_index("sp")
    me = tp * 4 + sp
    odd = lax.rem(sp, 2)
    pair = sp + 1 - 2 * odd

    small = [pltpu.make_async_copy(a, b, small_sem.at[i]) for i, (a, b) in enumerate(
        ((x_hbm, xb), (g1_hbm, g1), (g2_hbm, g2), (u_hbm, ub), (wb_hbm, wbb)))]

    def head_copy(j, h):
        a, b = ((wq_hbm, wq), (rel_hbm, rel), (wk_hbm, wk), (wv_hbm, wv))[j]
        return pltpu.make_async_copy(a.at[h], b.at[h], in_sem.at[j, h])

    weights = (
        pltpu.make_async_copy(wo_hbm, wo, w_sem.at[0]),
        pltpu.make_async_copy(wu_hbm.at[:, pl.ds(pl.multiple_of(sp * HID, 128), HID)], wu, w_sem.at[1]),
        pltpu.make_async_copy(wd_hbm.at[pl.ds(pl.multiple_of(sp * HID, 128), HID), :], wd, w_sem.at[2]),
    )

    def load(step, slot):
        @pl.when(step < BATCH)
        def _():
            pltpu.make_async_copy(k_hbm.at[step], ring.at[slot], ring_sem.at[slot]).start()

        @pl.when(jnp.logical_and(step >= BATCH, step < 2 * BATCH))
        def _():
            pltpu.make_async_copy(v_hbm.at[step - BATCH], ring.at[slot], ring_sem.at[slot]).start()

    for c in small:
        c.start()
    for j in range(2):
        for h in range(HEADS):
            head_copy(j, h).start()
    for i in range(FIRST):
        pltpu.make_async_copy(k_hbm.at[i], ring.at[i], ring_sem.at[i]).start()

    others = [(dt, ds) for dt in range(2) for ds in range(4) if (dt, ds) != (0, 0)]

    def peer(dt, ds):
        return lax.rem(tp + dt, 2), lax.rem(sp + ds, 4)

    def source(dt, ds):
        return lax.rem(tp + 2 - dt, 2), lax.rem(sp + 4 - ds, 4)

    barrier = pltpu.get_barrier_semaphore()
    for dt, ds in others:
        t, s = peer(dt, ds)
        pl.semaphore_signal(barrier, inc=1, device_id={"tp": t, "sp": s}, device_id_type=MESH)

    def remote(src, dst, send, recv, t, s):
        return pltpu.make_async_remote_copy(
            src_ref=src, dst_ref=dst, send_sem=send, recv_sem=recv, device_id={"tp": t, "sp": s}, device_id_type=MESH
        )

    def rows(g):
        return pl.ds(pl.multiple_of(g * GROWS, 8), GROWS)

    def pair_copy(g):
        return remote(rolled.at[:, rows(g), :], from_pair.at[:, rows(g), :], pair_s.at[g], pair_r.at[g], tp, pair)

    def far_copy(g, src=None):
        return remote((to_far if src is None else src).at[:, rows(g), :], from_far.at[:, rows(g), :], far_s.at[g], far_r.at[g], tp, 3 - sp)

    def stat_copy(g, ds):
        t, s = peer(0, ds)
        return remote(stat_out.at[rows(g), :], stat_in.at[ds - 1, rows(g), :], stat_s.at[g, ds - 1], stat_r.at[g, ds - 1], t, s)

    def ctx_copy(g, ds, sending):
        t, s = peer(0, ds)
        _, fs = source(0, ds)
        slot = sp if sending else fs
        return remote(ctx_in.at[slot, rows(g), :], ctx_in.at[slot, rows(g), :], ctx_s.at[g, ds - 1], ctx_r.at[g, ds - 1], t, s)

    def part_copy(g):
        return remote(part_out.at[g], part_in.at[g], part_s.at[g], part_r.at[g], 1 - tp, sp)

    def mlp_copy(g, j, sending):
        t, s = peer(*others[j])
        ft, fs = source(*others[j])
        slot = me if sending else ft * 4 + fs
        return remote(mlp_in.at[g, slot], mlp_in.at[g, slot], mlp_s.at[g, j], mlp_r.at[g, j], t, s)

    for c in small:
        c.wait()
    x = xb[...].astype(F32)
    for g in range(GROUPS):
        x1_ref[g] = x[PER * g : PER * g + PER, :]
    normed = rms_norm(x, g1[...].astype(F32).reshape(1, D))
    qf[...] = jnp.zeros_like(qf)
    for h in range(HEADS):
        head_copy(0, h).wait()
        q = jnp.dot(normed, wq[h], preferred_element_type=F32).astype(BF16).astype(F32)
        qc = (q + ub[h : h + 1, :].astype(F32)).astype(BF16).astype(F32)
        qp = (q + wbb[h : h + 1, :].astype(F32)).astype(BF16)
        qc_ref[h] = qc
        qf[h, pl.ds(h, BATCH, stride=8), :] = qc
        head_copy(1, h).wait()
        by_dist = lax.dot_general(qp, rel[h], NT, preferred_element_type=F32)
        for c in range(TILES):
            for s in range(GROUPS):
                row = s * GROWS + h * PER
                raw[c, row : row + PER, :] = by_dist[s * PER : s * PER + PER, c * 128 : c * 128 + 128]

    def lengths_of(group, count):
        seq = lax.rem(lax.broadcasted_iota(jnp.int32, (count, 128), 0), PER)
        out = jnp.zeros((count, 128), jnp.int32) + len_ref[PER * group]
        for i in range(1, PER):
            out = jnp.where(seq == i, len_ref[PER * group + i], out)
        return out

    lane8 = lax.broadcasted_iota(jnp.int32, (8, 128), 1)

    def roll(piece):
        r = lax.rem(lengths_of(lax.div(piece, GROWS // 8), 8), BLK)
        big, small_r = lax.div(r, 128), lax.rem(r, 128)
        sl = pl.ds(pl.multiple_of(piece * 8, 8), 8)
        idx = lax.rem(small_r - lane8 + 128, 128)
        tiles = [jnp.take_along_axis(raw[(TILES - c) % TILES, sl, :], idx, axis=1) for c in range(TILES)]
        for k in range(4):
            bit = lax.rem(lax.div(big, 1 << k), 2) == 1
            tiles = [jnp.where(bit, tiles[(c - (1 << k)) % TILES], tiles[c]) for c in range(TILES)]
        low = lane8 <= small_r
        for c in range(TILES):
            rolled[c, sl, :] = jnp.where(low, tiles[c], tiles[(c + 1) % TILES])

    def content(b):
        slot = lax.rem(b, RING)
        pltpu.make_async_copy(k_hbm.at[b], ring.at[slot], ring_sem.at[slot]).wait()
        sl = pl.ds(pl.multiple_of(b * 8, 8), 8)
        total = None
        for p in range(HEADS // 2):
            keys = jnp.concatenate([ring[slot, 2 * p], ring[slot, 2 * p + 1]], axis=1)
            query = jnp.concatenate([qf[2 * p, sl, :], qf[2 * p + 1, sl, :]], axis=1).astype(BF16)
            dots = lax.dot_general(query, keys, NT, preferred_element_type=F32)
            total = dots if total is None else total + dots
        first = lax.div(b, PER) * GROWS + lax.rem(b, PER)
        for c in range(TILES):
            score[c, pl.ds(first, HEADS, stride=PER), :] = total[:HEADS, c * 128 : c * 128 + 128]
        return slot

    lane24 = lax.broadcasted_iota(jnp.int32, (GROWS, 128), 1)

    def merge(g):
        pair_copy(g).wait()
        n = lengths_of(g, GROWS)
        r = lax.rem(n, BLK)
        last = lax.div(n, BLK) == 3
        for c in range(TILES):
            mine = jnp.logical_or(jnp.logical_and(last, lane24 + 128 * c <= r), odd == 0)
            to_far[c, rows(g), :] = jnp.where(mine, rolled[c, rows(g), :], from_pair[c, rows(g), :])

    def refill(b, slot):
        @pl.when(b <= RING - FIRST - 1)
        def _():
            for k in range(2):
                nxt = FIRST + 2 * b + k
                load(nxt, lax.rem(nxt, RING))

        @pl.when(b > RING - FIRST - 1)
        def _():
            load(b + RING, slot)

    pl.semaphore_wait(barrier, 7)

    def send(g):
        pair_copy(g).start()

        @pl.when(odd == 0)
        def _():
            far_copy(g, rolled).start()

    for b in range(3):
        slot = content(jnp.int32(b))
        for k in range(4):
            roll(4 * b + k)
        refill(jnp.int32(b), slot)
        send(b)
    send(3)

    def k_mid(b, _):
        slot = content(b)
        refill(b, slot)

        @pl.when(odd == 1)
        def _():
            @pl.when(b < 3 + GROUPS)
            def _():
                merge(b - 3)

            @pl.when(jnp.logical_and(b >= 4, b < 4 + GROUPS))
            def _():
                far_copy(b - 4).start()

        @pl.when(b == 4)
        def _():
            for j in (2, 3):
                for h in range(HEADS):
                    head_copy(j, h).start()

        @pl.when(b == 9)
        def _():
            for w in weights:
                w.start()

        return 0

    lax.fori_loop(3, 12, k_mid, 0)
    for h in range(HEADS):
        head_copy(2, h).wait()
        kn = jnp.dot(normed, wk[h], preferred_element_type=F32).astype(BF16).astype(F32)
        head_copy(3, h).wait()
        vn = jnp.dot(normed, wv[h], preferred_element_type=F32).astype(BF16).astype(F32)
        sn = jnp.broadcast_to(jnp.sum(qc_ref[h] * kn, axis=1, keepdims=True), (BATCH, 128))
        for s in range(GROUPS):
            row = s * GROWS + h * PER
            new_score[row : row + PER, :] = sn[s * PER : s * PER + PER, :]
            new_value[row : row + PER, :] = vn[s * PER : s * PER + PER, :]
    @pl.when(odd == 0)
    def _():
        for g in range(GROUPS):
            pair_copy(g).wait()

    def k_late(b, _):
        slot = content(b)
        refill(b, slot)
        return 0

    lax.fori_loop(12, BATCH, k_late, 0)

    lane6 = lax.broadcasted_iota(jnp.int32, (HEADS, 128), 1)
    head_row = lax.broadcasted_iota(jnp.int32, (HEADS, 128), 0)

    def softmax(b):
        sl = pl.ds(lax.div(b, PER) * GROWS + lax.rem(b, PER), HEADS, stride=PER)
        n = len_ref[b]
        r = lax.rem(n, BLK)
        block = lax.div(n, BLK)
        here = n - sp * BLK
        new = new_score[sl, :]
        own_a, pair_a = block - sp == sp, block - sp == pair
        own_b, pair_b = block - sp - 1 == sp, block - sp - 1 == pair
        sc = []
        for c in range(TILES):
            pos = lane6 + 128 * c
            own, near, far = rolled[c, sl, :], from_pair[c, sl, :], from_far[c, sl, :]
            rel_a = jnp.where(own_a, own, jnp.where(pair_a, near, far))
            rel_b = jnp.where(own_b, own, jnp.where(pair_b, near, far))
            rel_c = jnp.where(pos <= r, rel_a, rel_b)
            con = jnp.where(pos == here, new, score[c, sl, :])
            sc.append(jnp.where(pos <= here, (con + rel_c) * (HEAD**-0.5), MASKED))
        top = functools.reduce(jnp.maximum, sc)
        top = jnp.max(top, axis=1, keepdims=True)
        total = jnp.zeros((HEADS, 128), F32)
        at_new = jnp.zeros((HEADS, 128), F32)
        slot = lax.rem(b, 3)
        for c in range(TILES):
            pos = lane6 + 128 * c
            w = jnp.where(pos <= here, jnp.exp(sc[c] - top), 0.0)
            total = total + w
            at_new = at_new + jnp.where(pos == here, w.astype(BF16).astype(F32), 0.0)
            probs[slot, :, c * 128 : c * 128 + 128] = jnp.where(pos == here, 0.0, w)
        total = jnp.sum(total, axis=1, keepdims=True)
        at_new = jnp.sum(at_new, axis=1, keepdims=True)
        stat_out[sl, :] = jnp.where(lane6 < 64, top, total)
        new_prob[sl, :] = jnp.broadcast_to(at_new, (HEADS, 128))

    def attend(b):
        slot = lax.rem(b + BATCH, RING)
        pltpu.make_async_copy(v_hbm.at[b], ring.at[slot], ring_sem.at[slot]).wait()
        pb = probs[lax.rem(b, 3)].astype(BF16)
        out = jnp.zeros((HEADS, 128), F32)
        for p in range(HEADS // 2):
            values = jnp.concatenate([ring[slot, 2 * p], ring[slot, 2 * p + 1]], axis=1)
            dots = jnp.dot(pb, values, preferred_element_type=F32)
            out = jnp.where(head_row == 2 * p, dots[:, :128], jnp.where(head_row == 2 * p + 1, dots[:, 128:], out))
        ctx[pl.ds(lax.div(b, PER) * GROWS + lax.rem(b, PER), HEADS, stride=PER), :] = out
        return slot

    def send_stats(g):
        for ds in range(1, 4):
            stat_copy(g, ds).start()

    def send_ctx(g):
        for ds in range(1, 4):
            stat_copy(g, ds).wait()
        mine = stat_out[rows(g), :]
        top, total = mine[:, :1], mine[:, 64:65]
        all_top = top
        for ds in range(3):
            all_top = jnp.maximum(all_top, stat_in[ds, rows(g), :][:, :1])
        all_total = total * jnp.exp(top - all_top)
        for ds in range(3):
            got = stat_in[ds, rows(g), :]
            all_total = all_total + got[:, 64:65] * jnp.exp(got[:, :1] - all_top)
        scale = jnp.exp(top - all_top) / all_total
        ctx_in[sp, rows(g), :] = (ctx[rows(g), :] + new_prob[rows(g), :] * new_value[rows(g), :]) * scale
        for ds in range(1, 4):
            ctx_copy(g, ds, True).start()

    def project(g):
        for ds in range(1, 4):
            ctx_copy(g, ds, True).wait_send()
            ctx_copy(g, ds, False).wait_recv()
        whole = (ctx_in[0, rows(g), :] + ctx_in[1, rows(g), :]) + (ctx_in[2, rows(g), :] + ctx_in[3, rows(g), :])
        lhs = jnp.concatenate([whole[h * PER : h * PER + PER, :] for h in range(HEADS)], axis=1).astype(BF16)
        part_out[g] = jnp.dot(lhs, wo[...], preferred_element_type=F32)
        part_copy(g).start()

    def mlp(g):
        part_copy(g).wait()
        x1 = (x1_ref[g] + (part_out[g] + part_in[g])).astype(BF16).astype(F32)
        x1_ref[g] = x1
        up = jnp.dot(rms_norm(x1, g2[...].astype(F32).reshape(1, D)), wu[...], preferred_element_type=F32)
        act = jax.nn.gelu(up, approximate=True).astype(BF16)
        mlp_in[g, me] = jnp.dot(act, wd[...], preferred_element_type=F32)
        for j in range(7):
            mlp_copy(g, j, True).start()

    def finish(g):
        for j in range(7):
            mlp_copy(g, j, True).wait_send()
            mlp_copy(g, j, False).wait_recv()
        tot = mlp_in[g, 0]
        for k in range(1, 8):
            tot = tot + mlp_in[g, k]
        return x1_ref[g] + tot

    far_copy(0).wait()
    softmax(0)
    softmax(1)

    def v_step(b, _):
        g, i = lax.div(b, PER), lax.rem(b, PER)

        @pl.when(jnp.logical_and(i == 2, g < GROUPS - 1))
        def _():
            far_copy(g + 1).wait()

        slot = attend(b)
        softmax(b + 2)
        load(b + BATCH + RING, slot)

        @pl.when(b == 3)
        def _():
            for w in weights:
                w.wait()

        @pl.when(i == 1)
        def _():
            send_stats(g)

        @pl.when(i == 3)
        def _():
            send_ctx(g)

        @pl.when(jnp.logical_and(i == 2, g >= 1))
        def _():
            project(g - 1)

        @pl.when(jnp.logical_and(i == 1, g >= 2))
        def _():
            mlp(g - 2)

        return 0

    lax.fori_loop(0, BATCH - 2, v_step, 0)
    attend(jnp.int32(BATCH - 2))
    project(GROUPS - 2)
    attend(jnp.int32(BATCH - 1))
    send_ctx(GROUPS - 1)
    mlp(GROUPS - 2)
    project(GROUPS - 1)
    done = [finish(0), finish(1)]
    mlp(GROUPS - 1)
    done = done + [finish(2), finish(3)]
    out_ref[...] = jnp.concatenate(done, axis=0).astype(BF16)


def solution(mesh):
    spec_rows = P('dp', None)
    spec_cache = P('dp', 'sp', 'tp', None)
    in_specs = (spec_rows, spec_cache, spec_cache, P('dp'), P('sp', 'tp', None), P('tp', None), P('tp', None), P(None), P(None, 'tp', None), P(None, 'tp', None), P(None, 'tp', None), P('tp', None, None), P(None), P(None, 'tp'), P('tp', None))
    out_specs = spec_rows
    vm = pl.BlockSpec(memory_space=VMEM)
    hbm = pl.BlockSpec(memory_space=pl.ANY)
    smem = pl.BlockSpec(memory_space=pltpu.SMEM)
    dma = pltpu.SemaphoreType.DMA
    head_weight = VMEM((HEADS, D, HEAD), BF16)
    tiles = VMEM((TILES, ROWS, 128), F32)
    by_row = VMEM((ROWS, 128), F32)

    def layer_step(hidden, k_cache, v_cache, lengths, rel_table, u_bias, w_bias, g_attn, w_query, w_key, w_value, w_out, g_mlp, w_up, w_down):
        heads_first = lambda w: jnp.transpose(w, (1, 0, 2))
        return pl.pallas_call(
            fused_kernel,
            out_shape=jax.ShapeDtypeStruct((BATCH, D), BF16),
            in_specs=[smem] + [hbm] * 14,
            out_specs=vm,
            scratch_shapes=[
                VMEM((BATCH, D), BF16), VMEM((D,), BF16), VMEM((D,), BF16), VMEM((HEADS, HEAD), BF16), VMEM((HEADS, HEAD), BF16),
                head_weight, head_weight, head_weight, VMEM((HEADS, BLK, HEAD), BF16),
                VMEM((HEADS, 128, 128), F32), VMEM((HEADS, BATCH, 128), F32), tiles, by_row, by_row, by_row,
                VMEM((RING, HEADS, BLK, HEAD), BF16), VMEM((HEADS * HEAD, D), BF16), VMEM((D, HID), BF16), VMEM((HID, D), BF16),
                tiles, tiles, tiles, tiles, tiles, VMEM((3, HEADS, BLK), F32),
                by_row, VMEM((3, ROWS, 128), F32), by_row, VMEM((4, ROWS, 128), F32),
                VMEM((GROUPS, PER, D), F32), VMEM((GROUPS, PER, D), F32), VMEM((GROUPS, PER, D), F32), VMEM((GROUPS, 8, PER, D), F32),
                dma((5,)), dma((4, HEADS)), dma((RING,)), dma((3,)), dma((4,)), dma((4,)), dma((4,)), dma((4,)),
                dma((4, 3)), dma((4, 3)), dma((4, 3)), dma((4, 3)), dma((4,)), dma((4,)), dma((4, 7)), dma((4, 7)),
            ],
            compiler_params=pltpu.CompilerParams(vmem_limit_bytes=63 * 2**20, collective_id=0, has_side_effects=True),
            name="layer",
        )(
            lengths, hidden, g_attn, g_mlp, u_bias, w_bias,
            heads_first(w_query), heads_first(w_key), heads_first(w_value), heads_first(rel_table),
            jnp.transpose(k_cache, (0, 2, 1, 3)), jnp.transpose(v_cache, (0, 2, 1, 3)),
            w_out.reshape(HEADS * HEAD, D), w_up, w_down,
        )

    return jax.shard_map(layer_step, mesh=mesh, in_specs=in_specs, out_specs=out_specs, check_vma=False)
```

```python
import functools

import jax
import jax.numpy as jnp
from jax import lax
from jax.experimental import pallas as pl
from jax.experimental.pallas import tpu as pltpu
from jax.sharding import PartitionSpec as P

EPS = 1e-6
MASKED = -1e30
MESH = pl.DeviceIdType.MESH
F32 = jnp.float32
BF16 = jnp.bfloat16
VMEM = pltpu.VMEM
NT = (((1,), (1,)), ((), ()))

BATCH, HEADS, HEAD, BLK, D = 16, 6, 128, 2048, 1536
TILES = BLK // 128
GROUPS, PER = 4, 4
GROWS = HEADS * PER
ROWS = GROUPS * GROWS
RING = 8
FIRST = 3
HID = 768


def rms_norm(wide, gain):
    mean_sq = jnp.mean(wide * wide, axis=-1, keepdims=True)
    return (wide * lax.rsqrt(mean_sq + EPS) * gain).astype(BF16)


def fused_kernel(len_ref, x_hbm, g1_hbm, g2_hbm, u_hbm, wb_hbm, wq_hbm, wk_hbm, wv_hbm, rel_hbm, k_hbm, v_hbm, wo_hbm, wu_hbm, wd_hbm,
                 out_ref,
                 xb, g1, g2, ub, wbb, wq, wkv, kv, rel, qf, qc_ref, raw, new_score, new_value, new_prob,
                 ring, wo, wu, wd, score, rolled, from_pair, to_far, from_far, probs, stat_out, stat_in, ctx, ctx_in,
                 part_out, part_in, x1_ref, mlp_in,
                 small_sem, in_sem, kv_sem, kvp_s, kvp_r, ring_sem, w_sem, pair_s, pair_r, far_s, far_r, stat_s, stat_r, ctx_s, ctx_r,
                 part_s, part_r, mlp_s, mlp_r):
    tp, sp = lax.axis_index("tp"), lax.axis_index("sp")
    me = tp * 4 + sp
    odd = lax.rem(sp, 2)
    pair = sp + 1 - 2 * odd

    small = [pltpu.make_async_copy(a, b, small_sem.at[i]) for i, (a, b) in enumerate(
        ((x_hbm, xb), (g1_hbm, g1), (g2_hbm, g2), (u_hbm, ub), (wb_hbm, wbb)))]

    def head_copy(j, h):
        a, b = ((wq_hbm, wq), (rel_hbm, rel))[j]
        return pltpu.make_async_copy(a.at[h], b.at[h], in_sem.at[j, h])

    def kv_load(src, j):
        return pltpu.make_async_copy(src.at[lax.rem(sp, 2) * 3 + j], wkv.at[j], kv_sem.at[j])

    weights = (
        pltpu.make_async_copy(wo_hbm, wo, w_sem.at[0]),
        pltpu.make_async_copy(wu_hbm.at[:, pl.ds(pl.multiple_of(sp * HID, 128), HID)], wu, w_sem.at[1]),
        pltpu.make_async_copy(wd_hbm.at[pl.ds(pl.multiple_of(sp * HID, 128), HID), :], wd, w_sem.at[2]),
    )

    def load(step, slot):
        @pl.when(step < BATCH)
        def _():
            pltpu.make_async_copy(k_hbm.at[step], ring.at[slot], ring_sem.at[slot]).start()

        @pl.when(jnp.logical_and(step >= BATCH, step < 2 * BATCH))
        def _():
            pltpu.make_async_copy(v_hbm.at[step - BATCH], ring.at[slot], ring_sem.at[slot]).start()

    for c in small:
        c.start()
    for j in range(2):
        for h in range(HEADS):
            head_copy(j, h).start()

    @pl.when(sp < 2)
    def _():
        for j in range(3):
            kv_load(wk_hbm, j).start()

    @pl.when(sp >= 2)
    def _():
        for j in range(3):
            kv_load(wv_hbm, j).start()

    for i in range(FIRST):
        pltpu.make_async_copy(k_hbm.at[i], ring.at[i], ring_sem.at[i]).start()

    others = [(dt, ds) for dt in range(2) for ds in range(4) if (dt, ds) != (0, 0)]

    def peer(dt, ds):
        return lax.rem(tp + dt, 2), lax.rem(sp + ds, 4)

    def source(dt, ds):
        return lax.rem(tp + 2 - dt, 2), lax.rem(sp + 4 - ds, 4)

    barrier = pltpu.get_barrier_semaphore()
    for dt, ds in others:
        t, s = peer(dt, ds)
        pl.semaphore_signal(barrier, inc=1, device_id={"tp": t, "sp": s}, device_id_type=MESH)

    def remote(src, dst, send, recv, t, s):
        return pltpu.make_async_remote_copy(
            src_ref=src, dst_ref=dst, send_sem=send, recv_sem=recv, device_id={"tp": t, "sp": s}, device_id_type=MESH
        )

    def rows(g):
        return pl.ds(pl.multiple_of(g * GROWS, 8), GROWS)

    def pair_copy(g):
        return remote(rolled.at[:, rows(g), :], from_pair.at[:, rows(g), :], pair_s.at[g], pair_r.at[g], tp, pair)

    def far_copy(g, src=None):
        return remote((to_far if src is None else src).at[:, rows(g), :], from_far.at[:, rows(g), :], far_s.at[g], far_r.at[g], tp, 3 - sp)

    def kv_copy(ds, sending):
        t, s = peer(0, ds)
        _, fs = source(0, ds)
        part = kv.at[pl.ds((sp if sending else fs) * 3, 3)]
        return remote(part, part, kvp_s.at[ds - 1], kvp_r.at[ds - 1], t, s)

    def stat_copy(g, ds):
        t, s = peer(0, ds)
        return remote(stat_out.at[rows(g), :], stat_in.at[ds - 1, rows(g), :], stat_s.at[g, ds - 1], stat_r.at[g, ds - 1], t, s)

    def ctx_copy(g, ds, sending):
        t, s = peer(0, ds)
        _, fs = source(0, ds)
        slot = sp if sending else fs
        return remote(ctx_in.at[slot, rows(g), :], ctx_in.at[slot, rows(g), :], ctx_s.at[g, ds - 1], ctx_r.at[g, ds - 1], t, s)

    def part_copy(g):
        return remote(part_out.at[g], part_in.at[g], part_s.at[g], part_r.at[g], 1 - tp, sp)

    def mlp_copy(g, j, sending):
        t, s = peer(*others[j])
        ft, fs = source(*others[j])
        slot = me if sending else ft * 4 + fs
        return remote(mlp_in.at[g, slot], mlp_in.at[g, slot], mlp_s.at[g, j], mlp_r.at[g, j], t, s)

    for c in small:
        c.wait()
    x = xb[...].astype(F32)
    for g in range(GROUPS):
        x1_ref[g] = x[PER * g : PER * g + PER, :]
    normed = rms_norm(x, g1[...].astype(F32).reshape(1, D))
    qf[...] = jnp.zeros_like(qf)
    for h in range(HEADS):
        head_copy(0, h).wait()
        q = jnp.dot(normed, wq[h], preferred_element_type=F32).astype(BF16).astype(F32)
        qc = (q + ub[h : h + 1, :].astype(F32)).astype(BF16).astype(F32)
        qp = (q + wbb[h : h + 1, :].astype(F32)).astype(BF16)
        qc_ref[h] = qc
        qf[h, pl.ds(h, BATCH, stride=8), :] = qc
        head_copy(1, h).wait()
        by_dist = lax.dot_general(qp, rel[h], NT, preferred_element_type=F32)
        for c in range(TILES):
            for s in range(GROUPS):
                row = s * GROWS + h * PER
                raw[c, row : row + PER, :] = by_dist[s * PER : s * PER + PER, c * 128 : c * 128 + 128]

    def lengths_of(group, count):
        seq = lax.rem(lax.broadcasted_iota(jnp.int32, (count, 128), 0), PER)
        out = jnp.zeros((count, 128), jnp.int32) + len_ref[PER * group]
        for i in range(1, PER):
            out = jnp.where(seq == i, len_ref[PER * group + i], out)
        return out

    lane8 = lax.broadcasted_iota(jnp.int32, (8, 128), 1)

    def roll(piece):
        r = lax.rem(lengths_of(lax.div(piece, GROWS // 8), 8), BLK)
        big, small_r = lax.div(r, 128), lax.rem(r, 128)
        sl = pl.ds(pl.multiple_of(piece * 8, 8), 8)
        idx = lax.rem(small_r - lane8 + 128, 128)
        tiles = [jnp.take_along_axis(raw[(TILES - c) % TILES, sl, :], idx, axis=1) for c in range(TILES)]
        for k in range(4):
            bit = lax.rem(lax.div(big, 1 << k), 2) == 1
            tiles = [jnp.where(bit, tiles[(c - (1 << k)) % TILES], tiles[c]) for c in range(TILES)]
        low = lane8 <= small_r
        for c in range(TILES):
            rolled[c, sl, :] = jnp.where(low, tiles[c], tiles[(c + 1) % TILES])

    def content(b):
        slot = lax.rem(b, RING)
        pltpu.make_async_copy(k_hbm.at[b], ring.at[slot], ring_sem.at[slot]).wait()
        sl = pl.ds(pl.multiple_of(b * 8, 8), 8)
        total = None
        for p in range(HEADS // 2):
            keys = jnp.concatenate([ring[slot, 2 * p], ring[slot, 2 * p + 1]], axis=1)
            query = jnp.concatenate([qf[2 * p, sl, :], qf[2 * p + 1, sl, :]], axis=1).astype(BF16)
            dots = lax.dot_general(query, keys, NT, preferred_element_type=F32)
            total = dots if total is None else total + dots
        first = lax.div(b, PER) * GROWS + lax.rem(b, PER)
        for c in range(TILES):
            score[c, pl.ds(first, HEADS, stride=PER), :] = total[:HEADS, c * 128 : c * 128 + 128]
        return slot

    lane24 = lax.broadcasted_iota(jnp.int32, (GROWS, 128), 1)

    def merge(g):
        pair_copy(g).wait()
        n = lengths_of(g, GROWS)
        r = lax.rem(n, BLK)
        last = lax.div(n, BLK) == 3
        for c in range(TILES):
            mine = jnp.logical_or(jnp.logical_and(last, lane24 + 128 * c <= r), odd == 0)
            to_far[c, rows(g), :] = jnp.where(mine, rolled[c, rows(g), :], from_pair[c, rows(g), :])

    def refill(b, slot):
        @pl.when(b <= RING - FIRST - 1)
        def _():
            for k in range(2):
                nxt = FIRST + 2 * b + k
                load(nxt, lax.rem(nxt, RING))

        @pl.when(b > RING - FIRST - 1)
        def _():
            load(b + RING, slot)

    for j in range(3):
        kv_load(wk_hbm, j).wait()
        kv[sp * 3 + j] = jnp.dot(normed, wkv[j], preferred_element_type=F32).astype(BF16).astype(F32)

    def send(g):
        pair_copy(g).start()

        @pl.when(odd == 0)
        def _():
            far_copy(g, rolled).start()

    for b in range(3):
        slot = content(jnp.int32(b))
        for k in range(4):
            roll(4 * b + k)
        refill(jnp.int32(b), slot)
        if b == 0:
            pl.semaphore_wait(barrier, 7)
            for ds in range(1, 4):
                kv_copy(ds, True).start()
        send(b)
    send(3)

    def k_mid(b, _):
        slot = content(b)
        refill(b, slot)

        @pl.when(odd == 1)
        def _():
            @pl.when(b < 3 + GROUPS)
            def _():
                merge(b - 3)

            @pl.when(jnp.logical_and(b >= 4, b < 4 + GROUPS))
            def _():
                far_copy(b - 4).start()

        @pl.when(b == 9)
        def _():
            for w in weights:
                w.start()

        return 0

    lax.fori_loop(3, 12, k_mid, 0)
    @pl.when(odd == 0)
    def _():
        for g in range(GROUPS):
            pair_copy(g).wait()

    def k_late(b, _):
        slot = content(b)
        refill(b, slot)
        return 0

    lax.fori_loop(12, BATCH, k_late, 0)
    for ds in range(1, 4):
        kv_copy(ds, True).wait_send()
        kv_copy(ds, False).wait_recv()
    for h in range(HEADS):
        sn = jnp.broadcast_to(jnp.sum(qc_ref[h] * kv[h], axis=1, keepdims=True), (BATCH, 128))
        for s in range(GROUPS):
            row = s * GROWS + h * PER
            new_score[row : row + PER, :] = sn[s * PER : s * PER + PER, :]
            new_value[row : row + PER, :] = kv[HEADS + h, s * PER : s * PER + PER, :]

    lane6 = lax.broadcasted_iota(jnp.int32, (HEADS, 128), 1)
    head_row = lax.broadcasted_iota(jnp.int32, (HEADS, 128), 0)

    def softmax(b):
        sl = pl.ds(lax.div(b, PER) * GROWS + lax.rem(b, PER), HEADS, stride=PER)
        n = len_ref[b]
        r = lax.rem(n, BLK)
        block = lax.div(n, BLK)
        here = n - sp * BLK
        new = new_score[sl, :]
        own_a, pair_a = block - sp == sp, block - sp == pair
        own_b, pair_b = block - sp - 1 == sp, block - sp - 1 == pair
        sc = []
        for c in range(TILES):
            pos = lane6 + 128 * c
            own, near, far = rolled[c, sl, :], from_pair[c, sl, :], from_far[c, sl, :]
            rel_a = jnp.where(own_a, own, jnp.where(pair_a, near, far))
            rel_b = jnp.where(own_b, own, jnp.where(pair_b, near, far))
            rel_c = jnp.where(pos <= r, rel_a, rel_b)
            con = jnp.where(pos == here, new, score[c, sl, :])
            sc.append(jnp.where(pos <= here, (con + rel_c) * (HEAD**-0.5), MASKED))
        top = functools.reduce(jnp.maximum, sc)
        top = jnp.max(top, axis=1, keepdims=True)
        total = jnp.zeros((HEADS, 128), F32)
        at_new = jnp.zeros((HEADS, 128), F32)
        slot = lax.rem(b, 3)
        for c in range(TILES):
            pos = lane6 + 128 * c
            w = jnp.where(pos <= here, jnp.exp(sc[c] - top), 0.0)
            total = total + w
            at_new = at_new + jnp.where(pos == here, w.astype(BF16).astype(F32), 0.0)
            probs[slot, :, c * 128 : c * 128 + 128] = jnp.where(pos == here, 0.0, w)
        total = jnp.sum(total, axis=1, keepdims=True)
        at_new = jnp.sum(at_new, axis=1, keepdims=True)
        stat_out[sl, :] = jnp.where(lane6 < 64, top, total)
        new_prob[sl, :] = jnp.broadcast_to(at_new, (HEADS, 128))

    def attend(b):
        slot = lax.rem(b + BATCH, RING)
        pltpu.make_async_copy(v_hbm.at[b], ring.at[slot], ring_sem.at[slot]).wait()
        pb = probs[lax.rem(b, 3)].astype(BF16)
        out = jnp.zeros((HEADS, 128), F32)
        for p in range(HEADS // 2):
            values = jnp.concatenate([ring[slot, 2 * p], ring[slot, 2 * p + 1]], axis=1)
            dots = jnp.dot(pb, values, preferred_element_type=F32)
            out = jnp.where(head_row == 2 * p, dots[:, :128], jnp.where(head_row == 2 * p + 1, dots[:, 128:], out))
        ctx[pl.ds(lax.div(b, PER) * GROWS + lax.rem(b, PER), HEADS, stride=PER), :] = out
        return slot

    def send_stats(g):
        for ds in range(1, 4):
            stat_copy(g, ds).start()

    def send_ctx(g):
        for ds in range(1, 4):
            stat_copy(g, ds).wait()
        mine = stat_out[rows(g), :]
        top, total = mine[:, :1], mine[:, 64:65]
        all_top = top
        for ds in range(3):
            all_top = jnp.maximum(all_top, stat_in[ds, rows(g), :][:, :1])
        all_total = total * jnp.exp(top - all_top)
        for ds in range(3):
            got = stat_in[ds, rows(g), :]
            all_total = all_total + got[:, 64:65] * jnp.exp(got[:, :1] - all_top)
        scale = jnp.exp(top - all_top) / all_total
        ctx_in[sp, rows(g), :] = (ctx[rows(g), :] + new_prob[rows(g), :] * new_value[rows(g), :]) * scale
        for ds in range(1, 4):
            ctx_copy(g, ds, True).start()

    def project(g):
        for ds in range(1, 4):
            ctx_copy(g, ds, True).wait_send()
            ctx_copy(g, ds, False).wait_recv()
        whole = (ctx_in[0, rows(g), :] + ctx_in[1, rows(g), :]) + (ctx_in[2, rows(g), :] + ctx_in[3, rows(g), :])
        lhs = jnp.concatenate([whole[h * PER : h * PER + PER, :] for h in range(HEADS)], axis=1).astype(BF16)
        part_out[g] = jnp.dot(lhs, wo[...], preferred_element_type=F32)
        part_copy(g).start()

    def mlp(g):
        part_copy(g).wait()
        x1 = (x1_ref[g] + (part_out[g] + part_in[g])).astype(BF16).astype(F32)
        x1_ref[g] = x1
        up = jnp.dot(rms_norm(x1, g2[...].astype(F32).reshape(1, D)), wu[...], preferred_element_type=F32)
        act = jax.nn.gelu(up, approximate=True).astype(BF16)
        mlp_in[g, me] = jnp.dot(act, wd[...], preferred_element_type=F32)
        for j in range(7):
            mlp_copy(g, j, True).start()

    def finish(g):
        for j in range(7):
            mlp_copy(g, j, True).wait_send()
            mlp_copy(g, j, False).wait_recv()
        tot = mlp_in[g, 0]
        for k in range(1, 8):
            tot = tot + mlp_in[g, k]
        return x1_ref[g] + tot

    far_copy(0).wait()
    softmax(0)
    softmax(1)

    def v_step(b, _):
        g, i = lax.div(b, PER), lax.rem(b, PER)

        @pl.when(jnp.logical_and(i == 2, g < GROUPS - 1))
        def _():
            far_copy(g + 1).wait()

        slot = attend(b)
        softmax(b + 2)
        load(b + BATCH + RING, slot)

        @pl.when(b == 3)
        def _():
            for w in weights:
                w.wait()

        @pl.when(i == 1)
        def _():
            send_stats(g)

        @pl.when(i == 3)
        def _():
            send_ctx(g)

        @pl.when(jnp.logical_and(i == 2, g >= 1))
        def _():
            project(g - 1)

        @pl.when(b == 9)
        def _():
            mlp(0)

        return 0

    lax.fori_loop(0, BATCH - 2, v_step, 0)
    attend(jnp.int32(BATCH - 2))
    project(GROUPS - 2)
    attend(jnp.int32(BATCH - 1))
    send_ctx(3)
    mlp(1)
    project(3)
    mlp(2)
    done = [finish(0)]
    mlp(3)
    done = done + [finish(1), finish(2)]
    done = done + [finish(3)]
    out_ref[...] = jnp.concatenate(done, axis=0).astype(BF16)


def solution(mesh):
    spec_rows = P('dp', None)
    spec_cache = P('dp', 'sp', 'tp', None)
    in_specs = (spec_rows, spec_cache, spec_cache, P('dp'), P('sp', 'tp', None), P('tp', None), P('tp', None), P(None), P(None, 'tp', None), P(None, 'tp', None), P(None, 'tp', None), P('tp', None, None), P(None), P(None, 'tp'), P('tp', None))
    out_specs = spec_rows
    vm = pl.BlockSpec(memory_space=VMEM)
    hbm = pl.BlockSpec(memory_space=pl.ANY)
    smem = pl.BlockSpec(memory_space=pltpu.SMEM)
    dma = pltpu.SemaphoreType.DMA
    head_weight = VMEM((HEADS, D, HEAD), BF16)
    tiles = VMEM((TILES, ROWS, 128), F32)
    by_row = VMEM((ROWS, 128), F32)

    def layer_step(hidden, k_cache, v_cache, lengths, rel_table, u_bias, w_bias, g_attn, w_query, w_key, w_value, w_out, g_mlp, w_up, w_down):
        heads_first = lambda w: jnp.transpose(w, (1, 0, 2))
        return pl.pallas_call(
            fused_kernel,
            out_shape=jax.ShapeDtypeStruct((BATCH, D), BF16),
            in_specs=[smem] + [hbm] * 14,
            out_specs=vm,
            scratch_shapes=[
                VMEM((BATCH, D), BF16), VMEM((D,), BF16), VMEM((D,), BF16), VMEM((HEADS, HEAD), BF16), VMEM((HEADS, HEAD), BF16),
                head_weight, VMEM((3, D, HEAD), BF16), VMEM((2 * HEADS, BATCH, HEAD), F32), VMEM((HEADS, BLK, HEAD), BF16),
                VMEM((HEADS, 128, 128), F32), VMEM((HEADS, BATCH, 128), F32), tiles, by_row, by_row, by_row,
                VMEM((RING, HEADS, BLK, HEAD), BF16), VMEM((HEADS * HEAD, D), BF16), VMEM((D, HID), BF16), VMEM((HID, D), BF16),
                tiles, tiles, tiles, tiles, tiles, VMEM((3, HEADS, BLK), F32),
                by_row, VMEM((3, ROWS, 128), F32), by_row, VMEM((4, ROWS, 128), F32),
                VMEM((GROUPS, PER, D), F32), VMEM((GROUPS, PER, D), F32), VMEM((GROUPS, PER, D), F32), VMEM((GROUPS, 8, PER, D), F32),
                dma((5,)), dma((2, HEADS)), dma((3,)), dma((3,)), dma((3,)), dma((RING,)), dma((3,)), dma((4,)), dma((4,)), dma((4,)), dma((4,)),
                dma((4, 3)), dma((4, 3)), dma((4, 3)), dma((4, 3)), dma((4,)), dma((4,)), dma((4, 7)), dma((4, 7)),
            ],
            compiler_params=pltpu.CompilerParams(vmem_limit_bytes=63 * 2**20, collective_id=0, has_side_effects=True),
            name="layer",
        )(
            lengths, hidden, g_attn, g_mlp, u_bias, w_bias,
            heads_first(w_query), heads_first(w_key), heads_first(w_value), heads_first(rel_table),
            jnp.transpose(k_cache, (0, 2, 1, 3)), jnp.transpose(v_cache, (0, 2, 1, 3)),
            w_out.reshape(HEADS * HEAD, D), w_up, w_down,
        )

    return jax.shard_map(layer_step, mesh=mesh, in_specs=in_specs, out_specs=out_specs, check_vma=False)
```

```python
import functools

import jax
import jax.numpy as jnp
from jax import lax
from jax.experimental import pallas as pl
from jax.experimental.pallas import tpu as pltpu
from jax.sharding import PartitionSpec as P

EPS = 1e-6
MASKED = -1e30
MESH = pl.DeviceIdType.MESH
F32 = jnp.float32
BF16 = jnp.bfloat16
VMEM = pltpu.VMEM
NT = (((1,), (1,)), ((), ()))

BATCH, HEADS, HEAD, BLK, D = 16, 6, 128, 2048, 1536
TILES = BLK // 128
GROUPS, PER = 4, 4
GROWS = HEADS * PER
ROWS = GROUPS * GROWS
RING = 8
FIRST = 5
HID = 768


def rms_norm(wide, gain):
    mean_sq = jnp.mean(wide * wide, axis=-1, keepdims=True)
    return (wide * lax.rsqrt(mean_sq + EPS) * gain).astype(BF16)


def fused_kernel(len_hbm, x_hbm, g1_hbm, g2_hbm, u_hbm, wb_hbm, wq_hbm, wk_hbm, wv_hbm, rel_hbm, k_hbm, v_hbm, wo_hbm, wu_hbm, wd_hbm,
                 out_ref,
                 len_ref, xb, g1, g2, ub, wbb, wq, wkv, kv, rel, qf, qc_ref, raw, new_score, new_value, new_prob,
                 ring, wo, wu, wd, score, rolled, from_pair, to_far, from_far, probs, stat_out, stat_in, ctx, ctx_in,
                 part_out, part_in, x1_ref, mlp_in, x1_rows, rs_out, rs_in, ag,
                 small_sem, in_sem, kv_sem, kvp_s, kvp_r, ring_sem, w_sem, pair_s, pair_r, far_s, far_r, stat_s, stat_r, ctx_s, ctx_r,
                 part_s, part_r, mlp_s, mlp_r, rs_s, rs_r, ag_s, ag_r):
    tp, sp = lax.axis_index("tp"), lax.axis_index("sp")
    me = tp * 4 + sp
    odd = lax.rem(sp, 2)
    pair = sp + 1 - 2 * odd

    small = [pltpu.make_async_copy(a, b, small_sem.at[i]) for i, (a, b) in enumerate(
        ((len_hbm, len_ref), (x_hbm, xb), (g1_hbm, g1), (g2_hbm, g2), (u_hbm, ub), (wb_hbm, wbb)))]

    def head_copy(j, h):
        a, b = ((wq_hbm, wq), (rel_hbm, rel))[j]
        return pltpu.make_async_copy(a.at[h], b.at[h], in_sem.at[j, h])

    def kv_load(src, j):
        return pltpu.make_async_copy(src.at[lax.rem(sp, 2) * 3 + j], wkv.at[j], kv_sem.at[j])

    weights = (
        pltpu.make_async_copy(wo_hbm, wo, w_sem.at[0]),
        pltpu.make_async_copy(wu_hbm.at[:, pl.ds(pl.multiple_of(sp * HID, 128), HID)], wu, w_sem.at[1]),
        pltpu.make_async_copy(wd_hbm.at[pl.ds(pl.multiple_of(sp * HID, 128), HID), :], wd, w_sem.at[2]),
    )

    def load(step, slot):
        @pl.when(step < BATCH)
        def _():
            pltpu.make_async_copy(k_hbm.at[step], ring.at[slot], ring_sem.at[slot]).start()

        @pl.when(jnp.logical_and(step >= BATCH, step < 2 * BATCH))
        def _():
            pltpu.make_async_copy(v_hbm.at[step - BATCH], ring.at[slot], ring_sem.at[slot]).start()

    for c in small:
        c.start()
    for j in range(2):
        for h in range(HEADS):
            head_copy(j, h).start()

    @pl.when(sp < 2)
    def _():
        for j in range(3):
            kv_load(wk_hbm, j).start()

    @pl.when(sp >= 2)
    def _():
        for j in range(3):
            kv_load(wv_hbm, j).start()

    for i in range(FIRST - 3):
        pltpu.make_async_copy(k_hbm.at[i], ring.at[i], ring_sem.at[i]).start()

    others = [(dt, ds) for dt in range(2) for ds in range(4) if (dt, ds) != (0, 0)]

    def peer(dt, ds):
        return lax.rem(tp + dt, 2), lax.rem(sp + ds, 4)

    def source(dt, ds):
        return lax.rem(tp + 2 - dt, 2), lax.rem(sp + 4 - ds, 4)

    barrier = pltpu.get_barrier_semaphore()
    for dt, ds in others:
        t, s = peer(dt, ds)
        pl.semaphore_signal(barrier, inc=1, device_id={"tp": t, "sp": s}, device_id_type=MESH)

    def remote(src, dst, send, recv, t, s):
        return pltpu.make_async_remote_copy(
            src_ref=src, dst_ref=dst, send_sem=send, recv_sem=recv, device_id={"tp": t, "sp": s}, device_id_type=MESH
        )

    def rows(g):
        return pl.ds(pl.multiple_of(g * GROWS, 8), GROWS)

    def pair_copy(g):
        return remote(rolled.at[:, rows(g), :], from_pair.at[:, rows(g), :], pair_s.at[g], pair_r.at[g], tp, pair)

    def far_copy(g, src=None):
        return remote((to_far if src is None else src).at[:, rows(g), :], from_far.at[:, rows(g), :], far_s.at[g], far_r.at[g], tp, 3 - sp)

    def kv_copy(ds, sending):
        t, s = peer(0, ds)
        _, fs = source(0, ds)
        part = kv.at[pl.ds((sp if sending else fs) * 3, 3)]
        return remote(part, part, kvp_s.at[ds - 1], kvp_r.at[ds - 1], t, s)

    def stat_copy(g, ds):
        t, s = peer(0, ds)
        return remote(stat_out.at[rows(g), :], stat_in.at[ds - 1, rows(g), :], stat_s.at[g, ds - 1], stat_r.at[g, ds - 1], t, s)

    def ctx_copy(g, ds, sending):
        t, s = peer(0, ds)
        _, fs = source(0, ds)
        slot = sp if sending else fs
        return remote(ctx_in.at[slot, rows(g), :], ctx_in.at[slot, rows(g), :], ctx_s.at[g, ds - 1], ctx_r.at[g, ds - 1], t, s)

    def part_copy(g):
        return remote(part_out.at[g], part_in.at[g], part_s.at[g], part_r.at[g], 1 - tp, sp)

    def mlp_copy(g, j, sending):
        t, s = peer(*others[j])
        ft, fs = source(*others[j])
        slot = me if sending else ft * 4 + fs
        return remote(mlp_in.at[g, slot], mlp_in.at[g, slot], mlp_s.at[g, j], mlp_r.at[g, j], t, s)

    def rs_copy(j, sending):
        t, s = peer(*others[j])
        ft, fs = source(*others[j])
        slot = me if sending else ft * 4 + fs
        return remote(rs_out.at[t * 4 + s], rs_in.at[slot], rs_s.at[j], rs_r.at[j], t, s)

    def ag_copy(j, sending):
        t, s = peer(*others[j])
        ft, fs = source(*others[j])
        slot = me if sending else ft * 4 + fs
        return remote(ag.at[slot], ag.at[slot], ag_s.at[j], ag_r.at[j], t, s)

    for c in small:
        c.wait()
    x = xb[...].astype(F32)
    for g in range(GROUPS):
        x1_ref[g] = x[PER * g : PER * g + PER, :]
    normed = rms_norm(x, g1[...].astype(F32).reshape(1, D))
    qf[...] = jnp.zeros_like(qf)
    for h in range(HEADS):
        head_copy(0, h).wait()
        q = jnp.dot(normed, wq[h], preferred_element_type=F32).astype(BF16).astype(F32)
        qc = (q + ub[h : h + 1, :].astype(F32)).astype(BF16).astype(F32)
        qp = (q + wbb[h : h + 1, :].astype(F32)).astype(BF16)
        qc_ref[h] = qc
        qf[h, pl.ds(h, BATCH, stride=8), :] = qc
        if h % 2 == 0:
            i = FIRST - 3 + h // 2
            pltpu.make_async_copy(k_hbm.at[i], ring.at[i], ring_sem.at[i]).start()
        head_copy(1, h).wait()
        by_dist = lax.dot_general(qp, rel[h], NT, preferred_element_type=F32)
        for c in range(TILES):
            for s in range(GROUPS):
                row = s * GROWS + h * PER
                raw[c, row : row + PER, :] = by_dist[s * PER : s * PER + PER, c * 128 : c * 128 + 128]

    def lengths_of(group, count):
        seq = lax.rem(lax.broadcasted_iota(jnp.int32, (count, 128), 0), PER)
        out = jnp.zeros((count, 128), jnp.int32) + len_ref[PER * group]
        for i in range(1, PER):
            out = jnp.where(seq == i, len_ref[PER * group + i], out)
        return out

    lane8 = lax.broadcasted_iota(jnp.int32, (8, 128), 1)

    def roll(piece):
        r = lax.rem(lengths_of(lax.div(piece, GROWS // 8), 8), BLK)
        big, small_r = lax.div(r, 128), lax.rem(r, 128)
        sl = pl.ds(pl.multiple_of(piece * 8, 8), 8)
        idx = lax.rem(small_r - lane8 + 128, 128)
        tiles = [jnp.take_along_axis(raw[(TILES - c) % TILES, sl, :], idx, axis=1) for c in range(TILES)]
        for k in range(4):
            bit = lax.rem(lax.div(big, 1 << k), 2) == 1
            tiles = [jnp.where(bit, tiles[(c - (1 << k)) % TILES], tiles[c]) for c in range(TILES)]
        low = lane8 <= small_r
        for c in range(TILES):
            rolled[c, sl, :] = jnp.where(low, tiles[c], tiles[(c + 1) % TILES])

    def content(b):
        slot = lax.rem(b, RING)
        pltpu.make_async_copy(k_hbm.at[b], ring.at[slot], ring_sem.at[slot]).wait()
        sl = pl.ds(pl.multiple_of(b * 8, 8), 8)
        total = None
        for p in range(HEADS // 2):
            keys = jnp.concatenate([ring[slot, 2 * p], ring[slot, 2 * p + 1]], axis=1)
            query = jnp.concatenate([qf[2 * p, sl, :], qf[2 * p + 1, sl, :]], axis=1).astype(BF16)
            dots = lax.dot_general(query, keys, NT, preferred_element_type=F32)
            total = dots if total is None else total + dots
        first = lax.div(b, PER) * GROWS + lax.rem(b, PER)
        for c in range(TILES):
            score[c, pl.ds(first, HEADS, stride=PER), :] = total[:HEADS, c * 128 : c * 128 + 128]
        return slot

    lane24 = lax.broadcasted_iota(jnp.int32, (GROWS, 128), 1)

    def merge(g):
        pair_copy(g).wait()
        n = lengths_of(g, GROWS)
        r = lax.rem(n, BLK)
        last = lax.div(n, BLK) == 3
        for c in range(TILES):
            mine = jnp.logical_or(jnp.logical_and(last, lane24 + 128 * c <= r), odd == 0)
            to_far[c, rows(g), :] = jnp.where(mine, rolled[c, rows(g), :], from_pair[c, rows(g), :])

    def refill(b, slot):
        @pl.when(b <= RING - FIRST - 1)
        def _():
            for k in range(2):
                nxt = FIRST + 2 * b + k
                load(nxt, lax.rem(nxt, RING))

        @pl.when(b > RING - FIRST - 1)
        def _():
            load(b + RING, slot)

    for j in range(3):
        kv_load(wk_hbm, j).wait()
        kv[sp * 3 + j] = jnp.dot(normed, wkv[j], preferred_element_type=F32).astype(BF16).astype(F32)

    def send(g):
        pair_copy(g).start()

        @pl.when(odd == 0)
        def _():
            far_copy(g, rolled).start()

    for b in range(3):
        slot = content(jnp.int32(b))
        for k in range(4):
            roll(4 * b + k)
        refill(jnp.int32(b), slot)
        if b == 0:
            pl.semaphore_wait(barrier, 7)
            for ds in range(1, 4):
                kv_copy(ds, True).start()
        send(b)
    send(3)

    def k_mid(b, _):
        slot = content(b)
        refill(b, slot)

        @pl.when(odd == 1)
        def _():
            @pl.when(b < 3 + GROUPS)
            def _():
                merge(b - 3)

            @pl.when(jnp.logical_and(b >= 4, b < 4 + GROUPS))
            def _():
                far_copy(b - 4).start()

        @pl.when(b == 9)
        def _():
            weights[0].start()

        return 0

    lax.fori_loop(3, 12, k_mid, 0)
    @pl.when(odd == 0)
    def _():
        for g in range(GROUPS):
            pair_copy(g).wait()

    def k_late(b, _):
        slot = content(b)
        refill(b, slot)
        return 0

    lax.fori_loop(12, BATCH, k_late, 0)
    for ds in range(1, 4):
        kv_copy(ds, True).wait_send()
        kv_copy(ds, False).wait_recv()
    for h in range(HEADS):
        sn = jnp.broadcast_to(jnp.sum(qc_ref[h] * kv[h], axis=1, keepdims=True), (BATCH, 128))
        for s in range(GROUPS):
            row = s * GROWS + h * PER
            new_score[row : row + PER, :] = sn[s * PER : s * PER + PER, :]
            new_value[row : row + PER, :] = kv[HEADS + h, s * PER : s * PER + PER, :]

    lane6 = lax.broadcasted_iota(jnp.int32, (HEADS, 128), 1)
    head_row = lax.broadcasted_iota(jnp.int32, (HEADS, 128), 0)

    def softmax(b):
        sl = pl.ds(lax.div(b, PER) * GROWS + lax.rem(b, PER), HEADS, stride=PER)
        n = len_ref[b]
        r = lax.rem(n, BLK)
        block = lax.div(n, BLK)
        here = n - sp * BLK
        new = new_score[sl, :]
        own_a, pair_a = block - sp == sp, block - sp == pair
        own_b, pair_b = block - sp - 1 == sp, block - sp - 1 == pair
        sc = []
        for c in range(TILES):
            pos = lane6 + 128 * c
            own, near, far = rolled[c, sl, :], from_pair[c, sl, :], from_far[c, sl, :]
            rel_a = jnp.where(own_a, own, jnp.where(pair_a, near, far))
            rel_b = jnp.where(own_b, own, jnp.where(pair_b, near, far))
            rel_c = jnp.where(pos <= r, rel_a, rel_b)
            con = jnp.where(pos == here, new, score[c, sl, :])
            sc.append(jnp.where(pos <= here, (con + rel_c) * (HEAD**-0.5), MASKED))
        top = functools.reduce(jnp.maximum, sc)
        top = jnp.max(top, axis=1, keepdims=True)
        total = jnp.zeros((HEADS, 128), F32)
        at_new = jnp.zeros((HEADS, 128), F32)
        slot = lax.rem(b, 3)
        for c in range(TILES):
            pos = lane6 + 128 * c
            w = jnp.where(pos <= here, jnp.exp(sc[c] - top), 0.0)
            total = total + w
            at_new = at_new + jnp.where(pos == here, w.astype(BF16).astype(F32), 0.0)
            probs[slot, :, c * 128 : c * 128 + 128] = jnp.where(pos == here, 0.0, w)
        total = jnp.sum(total, axis=1, keepdims=True)
        at_new = jnp.sum(at_new, axis=1, keepdims=True)
        stat_out[sl, :] = jnp.where(lane6 < 64, top, total)
        new_prob[sl, :] = jnp.broadcast_to(at_new, (HEADS, 128))

    def attend(b):
        slot = lax.rem(b + BATCH, RING)
        pltpu.make_async_copy(v_hbm.at[b], ring.at[slot], ring_sem.at[slot]).wait()
        pb = probs[lax.rem(b, 3)].astype(BF16)
        out = jnp.zeros((HEADS, 128), F32)
        for p in range(HEADS // 2):
            values = jnp.concatenate([ring[slot, 2 * p], ring[slot, 2 * p + 1]], axis=1)
            dots = jnp.dot(pb, values, preferred_element_type=F32)
            out = jnp.where(head_row == 2 * p, dots[:, :128], jnp.where(head_row == 2 * p + 1, dots[:, 128:], out))
        ctx[pl.ds(lax.div(b, PER) * GROWS + lax.rem(b, PER), HEADS, stride=PER), :] = out
        return slot

    def send_stats(g):
        for ds in range(1, 4):
            stat_copy(g, ds).start()

    def send_ctx(g):
        for ds in range(1, 4):
            stat_copy(g, ds).wait()
        mine = stat_out[rows(g), :]
        top, total = mine[:, :1], mine[:, 64:65]
        all_top = top
        for ds in range(3):
            all_top = jnp.maximum(all_top, stat_in[ds, rows(g), :][:, :1])
        all_total = total * jnp.exp(top - all_top)
        for ds in range(3):
            got = stat_in[ds, rows(g), :]
            all_total = all_total + got[:, 64:65] * jnp.exp(got[:, :1] - all_top)
        scale = jnp.exp(top - all_top) / all_total
        ctx_in[sp, rows(g), :] = (ctx[rows(g), :] + new_prob[rows(g), :] * new_value[rows(g), :]) * scale
        for ds in range(1, 4):
            ctx_copy(g, ds, True).start()

    def project(g):
        for ds in range(1, 4):
            ctx_copy(g, ds, True).wait_send()
            ctx_copy(g, ds, False).wait_recv()
        whole = (ctx_in[0, rows(g), :] + ctx_in[1, rows(g), :]) + (ctx_in[2, rows(g), :] + ctx_in[3, rows(g), :])
        lhs = jnp.concatenate([whole[h * PER : h * PER + PER, :] for h in range(HEADS)], axis=1).astype(BF16)
        part_out[g] = jnp.dot(lhs, wo[...], preferred_element_type=F32)
        part_copy(g).start()

    def middle(g):
        part_copy(g).wait()
        return (x1_ref[g] + (part_out[g] + part_in[g])).astype(BF16).astype(F32)

    def hidden_layer(x1):
        up = jnp.dot(rms_norm(x1, g2[...].astype(F32).reshape(1, D)), wu[...], preferred_element_type=F32)
        act = jax.nn.gelu(up, approximate=True).astype(BF16)
        return jnp.dot(act, wd[...], preferred_element_type=F32)

    def mlp(g):
        x1 = middle(g)
        x1_ref[g] = x1
        mlp_in[g - 2, me] = hidden_layer(x1)
        for j in range(7):
            mlp_copy(g - 2, j, True).start()

    def first_mlp():
        x1 = jnp.concatenate([middle(0), middle(1)], axis=0)
        down = hidden_layer(x1)
        for k in range(8):
            x1_rows[k] = x1[k : k + 1, :]
            rs_out[k] = down[k : k + 1, :]
        for j in range(7):
            rs_copy(j, True).start()
        rs_in[me] = rs_out[me]

    def first_sum():
        for j in range(7):
            rs_copy(j, True).wait_send()
            rs_copy(j, False).wait_recv()
        tot = rs_in[0]
        for k in range(1, 8):
            tot = tot + rs_in[k]
        ag[me] = (x1_rows[me] + tot).astype(BF16).astype(F32)
        for j in range(7):
            ag_copy(j, True).start()

    def first_finish():
        for j in range(7):
            ag_copy(j, True).wait_send()
            ag_copy(j, False).wait_recv()
        return [ag[k] for k in range(8)]

    def finish(g):
        for j in range(7):
            mlp_copy(g - 2, j, True).wait_send()
            mlp_copy(g - 2, j, False).wait_recv()
        tot = mlp_in[g - 2, 0]
        for k in range(1, 8):
            tot = tot + mlp_in[g - 2, k]
        return x1_ref[g] + tot

    far_copy(0).wait()
    softmax(0)
    softmax(1)

    def v_step(b, _):
        g, i = lax.div(b, PER), lax.rem(b, PER)

        @pl.when(jnp.logical_and(i == 2, g < GROUPS - 1))
        def _():
            far_copy(g + 1).wait()

        slot = attend(b)
        softmax(b + 2)
        load(b + BATCH + RING, slot)

        @pl.when(b == 3)
        def _():
            weights[0].wait()

        @pl.when(i == 1)
        def _():
            send_stats(g)

        @pl.when(i == 3)
        def _():
            send_ctx(g)

        @pl.when(jnp.logical_and(i == 2, g >= 1))
        def _():
            project(g - 1)

        @pl.when(b == BATCH - RING - 1)
        def _():
            weights[1].start()
            weights[2].start()

        return 0

    lax.fori_loop(0, BATCH - 2, v_step, 0)
    attend(jnp.int32(BATCH - 2))
    project(GROUPS - 2)
    attend(jnp.int32(BATCH - 1))
    send_ctx(3)
    weights[1].wait()
    weights[2].wait()
    first_mlp()
    project(3)
    mlp(2)
    first_sum()
    mlp(3)
    done = first_finish()
    done = done + [finish(2)]
    done = done + [finish(3)]
    out_ref[...] = jnp.concatenate(done, axis=0).astype(BF16)


def solution(mesh):
    spec_rows = P('dp', None)
    spec_cache = P('dp', 'sp', 'tp', None)
    in_specs = (spec_rows, spec_cache, spec_cache, P('dp'), P('sp', 'tp', None), P('tp', None), P('tp', None), P(None), P(None, 'tp', None), P(None, 'tp', None), P(None, 'tp', None), P('tp', None, None), P(None), P(None, 'tp'), P('tp', None))
    out_specs = spec_rows
    vm = pl.BlockSpec(memory_space=VMEM)
    hbm = pl.BlockSpec(memory_space=pl.ANY)
    dma = pltpu.SemaphoreType.DMA
    head_weight = VMEM((HEADS, D, HEAD), BF16)
    tiles = VMEM((TILES, ROWS, 128), F32)
    by_row = VMEM((ROWS, 128), F32)

    def layer_step(hidden, k_cache, v_cache, lengths, rel_table, u_bias, w_bias, g_attn, w_query, w_key, w_value, w_out, g_mlp, w_up, w_down):
        heads_first = lambda w: jnp.transpose(w, (1, 0, 2))
        return pl.pallas_call(
            fused_kernel,
            out_shape=jax.ShapeDtypeStruct((BATCH, D), BF16),
            in_specs=[hbm] * 15,
            out_specs=vm,
            scratch_shapes=[
                pltpu.SMEM((BATCH,), jnp.int32), VMEM((BATCH, D), BF16), VMEM((D,), BF16), VMEM((D,), BF16), VMEM((HEADS, HEAD), BF16), VMEM((HEADS, HEAD), BF16),
                head_weight, VMEM((3, D, HEAD), BF16), VMEM((2 * HEADS, BATCH, HEAD), F32), VMEM((HEADS, BLK, HEAD), BF16),
                VMEM((HEADS, 128, 128), F32), VMEM((HEADS, BATCH, 128), F32), tiles, by_row, by_row, by_row,
                VMEM((RING, HEADS, BLK, HEAD), BF16), VMEM((HEADS * HEAD, D), BF16), VMEM((D, HID), BF16), VMEM((HID, D), BF16),
                tiles, tiles, tiles, tiles, tiles, VMEM((3, HEADS, BLK), F32),
                by_row, VMEM((3, ROWS, 128), F32), by_row, VMEM((4, ROWS, 128), F32),
                VMEM((GROUPS, PER, D), F32), VMEM((GROUPS, PER, D), F32), VMEM((GROUPS, PER, D), F32), VMEM((2, 8, PER, D), F32),
                VMEM((8, 1, D), F32), VMEM((8, 1, D), F32), VMEM((8, 1, D), F32), VMEM((8, 1, D), F32),
                dma((6,)), dma((2, HEADS)), dma((3,)), dma((3,)), dma((3,)), dma((RING,)), dma((3,)), dma((4,)), dma((4,)), dma((4,)), dma((4,)),
                dma((4, 3)), dma((4, 3)), dma((4, 3)), dma((4, 3)), dma((4,)), dma((4,)), dma((2, 7)), dma((2, 7)), dma((7,)), dma((7,)), dma((7,)), dma((7,)),
            ],
            compiler_params=pltpu.CompilerParams(vmem_limit_bytes=63 * 2**20, collective_id=0, has_side_effects=True),
            name="layer",
        )(
            lengths, hidden, g_attn, g_mlp, u_bias, w_bias,
            heads_first(w_query), heads_first(w_key), heads_first(w_value), heads_first(rel_table),
            jnp.transpose(k_cache, (0, 2, 1, 3)), jnp.transpose(v_cache, (0, 2, 1, 3)),
            w_out.reshape(HEADS * HEAD, D), w_up, w_down,
        )

    return jax.shard_map(layer_step, mesh=mesh, in_specs=in_specs, out_specs=out_specs, check_vma=False)
```

```python
import functools

import jax
import jax.numpy as jnp
from jax import lax
from jax.experimental import pallas as pl
from jax.experimental.pallas import tpu as pltpu
from jax.sharding import PartitionSpec as P

EPS = 1e-6
MASKED = -1e30
MESH = pl.DeviceIdType.MESH
F32 = jnp.float32
BF16 = jnp.bfloat16
VMEM = pltpu.VMEM
NT = (((1,), (1,)), ((), ()))

BATCH, HEADS, HEAD, BLK, D = 16, 6, 128, 2048, 1536
TILES = BLK // 128
GROUPS, PER = 4, 4
GROWS = HEADS * PER
ROWS = GROUPS * GROWS
RING = 8
FIRST = 5
FIRST_SEND = 9
HID = 768


def rms_norm(wide, gain):
    mean_sq = jnp.mean(wide * wide, axis=-1, keepdims=True)
    return (wide * lax.rsqrt(mean_sq + EPS) * gain).astype(BF16)


def fused_kernel(len_hbm, x_hbm, g1_hbm, g2_hbm, u_hbm, wb_hbm, wq_hbm, wk_hbm, wv_hbm, rel_hbm, k_hbm, v_hbm, wo_hbm, wu_hbm, wd_hbm,
                 out_ref,
                 len_ref, xb, g1, g2, ub, wbb, wq, wkv, kv, rel, qf, qc_ref, raw, new_score, new_value, new_prob,
                 ring, wo, wu, wd, score, rolled, from_pair, to_far, from_far, probs, stat_out, stat_in, ctx, ctx_in,
                 part_out, part_in, x1_ref, mlp_in, x1_rows, rs_out, rs_in, ag,
                 small_sem, in_sem, kv_sem, kvp_s, kvp_r, ring_sem, w_sem, pair_s, pair_r, far_s, far_r, stat_s, stat_r, ctx_s, ctx_r,
                 part_s, part_r, mlp_s, mlp_r, rs_s, rs_r, ag_s, ag_r):
    tp, sp = lax.axis_index("tp"), lax.axis_index("sp")
    me = tp * 4 + sp
    odd = lax.rem(sp, 2)
    pair = sp + 1 - 2 * odd

    small = [pltpu.make_async_copy(a, b, small_sem.at[i]) for i, (a, b) in enumerate(
        ((len_hbm, len_ref), (x_hbm, xb), (g1_hbm, g1), (g2_hbm, g2), (u_hbm, ub), (wb_hbm, wbb)))]

    def head_copy(j, h):
        a, b = ((wq_hbm, wq), (rel_hbm, rel))[j]
        return pltpu.make_async_copy(a.at[h], b.at[h], in_sem.at[j, h])

    def kv_load(src, j):
        return pltpu.make_async_copy(src.at[lax.rem(sp, 2) * 3 + j], wkv.at[j], kv_sem.at[j])

    weights = (
        pltpu.make_async_copy(wo_hbm, wo, w_sem.at[0]),
        pltpu.make_async_copy(wu_hbm.at[:, pl.ds(pl.multiple_of(sp * HID, 128), HID)], wu, w_sem.at[1]),
        pltpu.make_async_copy(wd_hbm.at[pl.ds(pl.multiple_of(sp * HID, 128), HID), :], wd, w_sem.at[2]),
    )

    def load(step, slot):
        @pl.when(step < BATCH)
        def _():
            pltpu.make_async_copy(k_hbm.at[step], ring.at[slot], ring_sem.at[slot]).start()

        @pl.when(jnp.logical_and(step >= BATCH, step < 2 * BATCH))
        def _():
            pltpu.make_async_copy(v_hbm.at[step - BATCH], ring.at[slot], ring_sem.at[slot]).start()

    for c in small:
        c.start()
    for j in range(2):
        for h in range(HEADS):
            head_copy(j, h).start()

    @pl.when(sp < 2)
    def _():
        for j in range(3):
            kv_load(wk_hbm, j).start()

    @pl.when(sp >= 2)
    def _():
        for j in range(3):
            kv_load(wv_hbm, j).start()

    for i in range(FIRST - 3):
        pltpu.make_async_copy(k_hbm.at[i], ring.at[i], ring_sem.at[i]).start()

    others = [(dt, ds) for dt in range(2) for ds in range(4) if (dt, ds) != (0, 0)]

    def peer(dt, ds):
        return lax.rem(tp + dt, 2), lax.rem(sp + ds, 4)

    def source(dt, ds):
        return lax.rem(tp + 2 - dt, 2), lax.rem(sp + 4 - ds, 4)

    barrier = pltpu.get_barrier_semaphore()
    for dt, ds in others:
        t, s = peer(dt, ds)
        pl.semaphore_signal(barrier, inc=1, device_id={"tp": t, "sp": s}, device_id_type=MESH)

    def remote(src, dst, send, recv, t, s):
        return pltpu.make_async_remote_copy(
            src_ref=src, dst_ref=dst, send_sem=send, recv_sem=recv, device_id={"tp": t, "sp": s}, device_id_type=MESH
        )

    def rows(g):
        return pl.ds(pl.multiple_of(g * GROWS, 8), GROWS)

    def pair_copy(g):
        return remote(rolled.at[:, rows(g), :], from_pair.at[:, rows(g), :], pair_s.at[g], pair_r.at[g], tp, pair)

    def far_copy(g, src=None):
        return remote((to_far if src is None else src).at[:, rows(g), :], from_far.at[:, rows(g), :], far_s.at[g], far_r.at[g], tp, 3 - sp)

    def kv_copy(ds, sending):
        t, s = peer(0, ds)
        _, fs = source(0, ds)
        part = kv.at[pl.ds((sp if sending else fs) * 3, 3)]
        return remote(part, part, kvp_s.at[ds - 1], kvp_r.at[ds - 1], t, s)

    def stat_copy(g, ds):
        t, s = peer(0, ds)
        return remote(stat_out.at[rows(g), :], stat_in.at[ds - 1, rows(g), :], stat_s.at[g, ds - 1], stat_r.at[g, ds - 1], t, s)

    def ctx_copy(g, ds, sending):
        t, s = peer(0, ds)
        _, fs = source(0, ds)
        slot = sp if sending else fs
        return remote(ctx_in.at[slot, rows(g), :], ctx_in.at[slot, rows(g), :], ctx_s.at[g, ds - 1], ctx_r.at[g, ds - 1], t, s)

    def part_copy(g):
        return remote(part_out.at[g], part_in.at[g], part_s.at[g], part_r.at[g], 1 - tp, sp)

    def mlp_copy(g, j, sending):
        t, s = peer(*others[j])
        ft, fs = source(*others[j])
        slot = me if sending else ft * 4 + fs
        return remote(mlp_in.at[g, slot], mlp_in.at[g, slot], mlp_s.at[g, j], mlp_r.at[g, j], t, s)

    def rs_copy(j, sending):
        t, s = peer(*others[j])
        ft, fs = source(*others[j])
        slot = me if sending else ft * 4 + fs
        return remote(rs_out.at[t * 4 + s], rs_in.at[slot], rs_s.at[j], rs_r.at[j], t, s)

    def ag_copy(j, sending):
        t, s = peer(*others[j])
        ft, fs = source(*others[j])
        slot = me if sending else ft * 4 + fs
        return remote(ag.at[slot], ag.at[slot], ag_s.at[j], ag_r.at[j], t, s)

    for c in small:
        c.wait()
    x = xb[...].astype(F32)
    for g in range(GROUPS):
        x1_ref[g] = x[PER * g : PER * g + PER, :]
    normed = rms_norm(x, g1[...].astype(F32).reshape(1, D))
    qf[...] = jnp.zeros_like(qf)
    for h in range(HEADS):
        head_copy(0, h).wait()
        q = jnp.dot(normed, wq[h], preferred_element_type=F32).astype(BF16).astype(F32)
        qc = (q + ub[h : h + 1, :].astype(F32)).astype(BF16).astype(F32)
        qp = (q + wbb[h : h + 1, :].astype(F32)).astype(BF16)
        qc_ref[h] = qc
        qf[h, pl.ds(h, BATCH, stride=8), :] = qc
        if h % 2 == 0:
            i = FIRST - 3 + h // 2
            pltpu.make_async_copy(k_hbm.at[i], ring.at[i], ring_sem.at[i]).start()
        head_copy(1, h).wait()
        by_dist = lax.dot_general(qp, rel[h], NT, preferred_element_type=F32)
        for c in range(TILES):
            for s in range(GROUPS):
                row = s * GROWS + h * PER
                raw[c, row : row + PER, :] = by_dist[s * PER : s * PER + PER, c * 128 : c * 128 + 128]

    def lengths_of(group, count):
        seq = lax.rem(lax.broadcasted_iota(jnp.int32, (count, 128), 0), PER)
        out = jnp.zeros((count, 128), jnp.int32) + len_ref[PER * group]
        for i in range(1, PER):
            out = jnp.where(seq == i, len_ref[PER * group + i], out)
        return out

    lane8 = lax.broadcasted_iota(jnp.int32, (8, 128), 1)

    def roll(piece):
        r = lax.rem(lengths_of(lax.div(piece, GROWS // 8), 8), BLK)
        big, small_r = lax.div(r, 128), lax.rem(r, 128)
        sl = pl.ds(pl.multiple_of(piece * 8, 8), 8)
        idx = lax.rem(small_r - lane8 + 128, 128)
        tiles = [jnp.take_along_axis(raw[(TILES - c) % TILES, sl, :], idx, axis=1) for c in range(TILES)]
        for k in range(4):
            bit = lax.rem(lax.div(big, 1 << k), 2) == 1
            tiles = [jnp.where(bit, tiles[(c - (1 << k)) % TILES], tiles[c]) for c in range(TILES)]
        low = lane8 <= small_r
        for c in range(TILES):
            rolled[c, sl, :] = jnp.where(low, tiles[c], tiles[(c + 1) % TILES])

    def content(b):
        slot = lax.rem(b, RING)
        pltpu.make_async_copy(k_hbm.at[b], ring.at[slot], ring_sem.at[slot]).wait()
        sl = pl.ds(pl.multiple_of(b * 8, 8), 8)
        total = None
        for p in range(HEADS // 2):
            keys = jnp.concatenate([ring[slot, 2 * p], ring[slot, 2 * p + 1]], axis=1)
            query = jnp.concatenate([qf[2 * p, sl, :], qf[2 * p + 1, sl, :]], axis=1).astype(BF16)
            dots = lax.dot_general(query, keys, NT, preferred_element_type=F32)
            total = dots if total is None else total + dots
        first = lax.div(b, PER) * GROWS + lax.rem(b, PER)
        for c in range(TILES):
            score[c, pl.ds(first, HEADS, stride=PER), :] = total[:HEADS, c * 128 : c * 128 + 128]
        return slot

    lane24 = lax.broadcasted_iota(jnp.int32, (GROWS, 128), 1)

    def merge(g):
        pair_copy(g).wait()
        n = lengths_of(g, GROWS)
        r = lax.rem(n, BLK)
        last = lax.div(n, BLK) == 3
        for c in range(TILES):
            mine = jnp.logical_or(jnp.logical_and(last, lane24 + 128 * c <= r), odd == 0)
            to_far[c, rows(g), :] = jnp.where(mine, rolled[c, rows(g), :], from_pair[c, rows(g), :])

    def refill(b, slot):
        @pl.when(b <= RING - FIRST - 1)
        def _():
            for k in range(2):
                nxt = FIRST + 2 * b + k
                load(nxt, lax.rem(nxt, RING))

        @pl.when(b > RING - FIRST - 1)
        def _():
            load(b + RING, slot)

    for j in range(3):
        kv_load(wk_hbm, j).wait()
        kv[sp * 3 + j] = jnp.dot(normed, wkv[j], preferred_element_type=F32).astype(BF16).astype(F32)

    def send(g):
        pair_copy(g).start()

        @pl.when(odd == 0)
        def _():
            far_copy(g, rolled).start()

    for b in range(3):
        slot = content(jnp.int32(b))
        for k in range(4):
            roll(4 * b + k)
        refill(jnp.int32(b), slot)
        if b == 0:
            pl.semaphore_wait(barrier, 7)
            for ds in range(1, 4):
                kv_copy(ds, True).start()
        send(b)
    send(3)

    def k_mid(b, _):
        slot = content(b)
        refill(b, slot)

        @pl.when(odd == 1)
        def _():
            @pl.when(b < 3 + GROUPS)
            def _():
                merge(b - 3)

            @pl.when(jnp.logical_and(b >= 4, b < 4 + GROUPS))
            def _():
                far_copy(b - 4).start()

        @pl.when(b == 9)
        def _():
            weights[0].start()

        return 0

    lax.fori_loop(3, 12, k_mid, 0)
    @pl.when(odd == 0)
    def _():
        for g in range(GROUPS):
            pair_copy(g).wait()

    def k_late(b, _):
        slot = content(b)
        refill(b, slot)
        return 0

    lax.fori_loop(12, BATCH, k_late, 0)
    for ds in range(1, 4):
        kv_copy(ds, True).wait_send()
        kv_copy(ds, False).wait_recv()
    for h in range(HEADS):
        sn = jnp.broadcast_to(jnp.sum(qc_ref[h] * kv[h], axis=1, keepdims=True), (BATCH, 128))
        for s in range(GROUPS):
            row = s * GROWS + h * PER
            new_score[row : row + PER, :] = sn[s * PER : s * PER + PER, :]
            new_value[row : row + PER, :] = kv[HEADS + h, s * PER : s * PER + PER, :]

    lane6 = lax.broadcasted_iota(jnp.int32, (HEADS, 128), 1)
    head_row = lax.broadcasted_iota(jnp.int32, (HEADS, 128), 0)

    def softmax(b):
        sl = pl.ds(lax.div(b, PER) * GROWS + lax.rem(b, PER), HEADS, stride=PER)
        n = len_ref[b]
        r = lax.rem(n, BLK)
        block = lax.div(n, BLK)
        here = n - sp * BLK
        new = new_score[sl, :]
        own_a, pair_a = block - sp == sp, block - sp == pair
        own_b, pair_b = block - sp - 1 == sp, block - sp - 1 == pair
        sc = []
        for c in range(TILES):
            pos = lane6 + 128 * c
            own, near, far = rolled[c, sl, :], from_pair[c, sl, :], from_far[c, sl, :]
            rel_a = jnp.where(own_a, own, jnp.where(pair_a, near, far))
            rel_b = jnp.where(own_b, own, jnp.where(pair_b, near, far))
            rel_c = jnp.where(pos <= r, rel_a, rel_b)
            con = jnp.where(pos == here, new, score[c, sl, :])
            sc.append(jnp.where(pos <= here, (con + rel_c) * (HEAD**-0.5), MASKED))
        top = functools.reduce(jnp.maximum, sc)
        top = jnp.max(top, axis=1, keepdims=True)
        total = jnp.zeros((HEADS, 128), F32)
        at_new = jnp.zeros((HEADS, 128), F32)
        slot = lax.rem(b, 4)
        for c in range(TILES):
            pos = lane6 + 128 * c
            w = jnp.where(pos <= here, jnp.exp(sc[c] - top), 0.0)
            total = total + w
            at_new = at_new + jnp.where(pos == here, w.astype(BF16).astype(F32), 0.0)
            probs[slot, :, c * 128 : c * 128 + 128] = jnp.where(pos == here, 0.0, w)
        total = jnp.sum(total, axis=1, keepdims=True)
        at_new = jnp.sum(at_new, axis=1, keepdims=True)
        stat_out[sl, :] = jnp.where(lane6 < 64, top, total)
        new_prob[sl, :] = jnp.broadcast_to(at_new, (HEADS, 128))

    def attend(b):
        slot = lax.rem(b + BATCH, RING)
        pltpu.make_async_copy(v_hbm.at[b], ring.at[slot], ring_sem.at[slot]).wait()
        pb = probs[lax.rem(b, 4)].astype(BF16)
        out = jnp.zeros((HEADS, 128), F32)
        for p in range(HEADS // 2):
            values = jnp.concatenate([ring[slot, 2 * p], ring[slot, 2 * p + 1]], axis=1)
            dots = jnp.dot(pb, values, preferred_element_type=F32)
            out = jnp.where(head_row == 2 * p, dots[:, :128], jnp.where(head_row == 2 * p + 1, dots[:, 128:], out))
        ctx[pl.ds(lax.div(b, PER) * GROWS + lax.rem(b, PER), HEADS, stride=PER), :] = out
        return slot

    def send_stats(g):
        for ds in range(1, 4):
            stat_copy(g, ds).start()

    def send_ctx(g):
        for ds in range(1, 4):
            stat_copy(g, ds).wait()
        mine = stat_out[rows(g), :]
        top, total = mine[:, :1], mine[:, 64:65]
        all_top = top
        for ds in range(3):
            all_top = jnp.maximum(all_top, stat_in[ds, rows(g), :][:, :1])
        all_total = total * jnp.exp(top - all_top)
        for ds in range(3):
            got = stat_in[ds, rows(g), :]
            all_total = all_total + got[:, 64:65] * jnp.exp(got[:, :1] - all_top)
        scale = jnp.exp(top - all_top) / all_total
        ctx_in[sp, rows(g), :] = (ctx[rows(g), :] + new_prob[rows(g), :] * new_value[rows(g), :]) * scale
        for ds in range(1, 4):
            ctx_copy(g, ds, True).start()

    def project(g):
        for ds in range(1, 4):
            ctx_copy(g, ds, True).wait_send()
            ctx_copy(g, ds, False).wait_recv()
        whole = (ctx_in[0, rows(g), :] + ctx_in[1, rows(g), :]) + (ctx_in[2, rows(g), :] + ctx_in[3, rows(g), :])
        lhs = jnp.concatenate([whole[h * PER : h * PER + PER, :] for h in range(HEADS)], axis=1).astype(BF16)
        part_out[g] = jnp.dot(lhs, wo[...], preferred_element_type=F32)
        part_copy(g).start()

    def middle(g):
        part_copy(g).wait()
        return (x1_ref[g] + (part_out[g] + part_in[g])).astype(BF16).astype(F32)

    def hidden_layer(x1):
        up = jnp.dot(rms_norm(x1, g2[...].astype(F32).reshape(1, D)), wu[...], preferred_element_type=F32)
        act = jax.nn.gelu(up, approximate=True).astype(BF16)
        return jnp.dot(act, wd[...], preferred_element_type=F32)

    def mlp(g):
        x1 = middle(g)
        x1_ref[g] = x1
        mlp_in[g - 2, me] = hidden_layer(x1)
        for j in range(7):
            mlp_copy(g - 2, j, True).start()

    def first_mlp():
        x1 = jnp.concatenate([middle(0), middle(1)], axis=0)
        down = hidden_layer(x1)
        for k in range(8):
            x1_rows[k] = x1[k : k + 1, :]
            rs_out[k] = down[k : k + 1, :]
        for j in range(7):
            rs_copy(j, True).start()
        rs_in[me] = rs_out[me]

    def first_sum():
        for j in range(7):
            rs_copy(j, True).wait_send()
            rs_copy(j, False).wait_recv()
        tot = rs_in[0]
        for k in range(1, 8):
            tot = tot + rs_in[k]
        ag[me] = (x1_rows[me] + tot).astype(BF16).astype(F32)
        for j in range(7):
            ag_copy(j, True).start()

    def first_finish():
        for j in range(7):
            ag_copy(j, True).wait_send()
            ag_copy(j, False).wait_recv()
        return [ag[k] for k in range(8)]

    def finish(g):
        for j in range(7):
            mlp_copy(g - 2, j, True).wait_send()
            mlp_copy(g - 2, j, False).wait_recv()
        tot = mlp_in[g - 2, 0]
        for k in range(1, 8):
            tot = tot + mlp_in[g - 2, k]
        return x1_ref[g] + tot

    far_copy(0).wait()
    softmax(0)
    softmax(1)
    softmax(2)

    def v_step(b, _):
        g, i = lax.div(b, PER), lax.rem(b, PER)

        @pl.when(jnp.logical_and(i == 1, g < GROUPS - 1))
        def _():
            far_copy(g + 1).wait()

        slot = attend(b)
        softmax(b + 3)
        load(b + BATCH + RING, slot)

        @pl.when(b == 3)
        def _():
            weights[0].wait()

        @pl.when(i == 0)
        def _():
            send_stats(g)

        @pl.when(jnp.logical_and(b >= FIRST_SEND, b < FIRST_SEND + GROUPS - 1))
        def _():
            send_ctx(b - FIRST_SEND)

        @pl.when(jnp.logical_and(b >= FIRST_SEND + 3, b < BATCH - 3))
        def _():
            project(b - FIRST_SEND - 3)

        @pl.when(b == BATCH - RING - 1)
        def _():
            weights[1].start()
            weights[2].start()

        return 0

    lax.fori_loop(0, BATCH - 3, v_step, 0)
    attend(jnp.int32(BATCH - 3))
    project(GROUPS - 3)
    attend(jnp.int32(BATCH - 2))
    project(GROUPS - 2)
    attend(jnp.int32(BATCH - 1))
    send_ctx(3)
    weights[1].wait()
    weights[2].wait()
    first_mlp()
    project(3)
    mlp(2)
    first_sum()
    mlp(3)
    done = first_finish()
    done = done + [finish(2)]
    done = done + [finish(3)]
    out_ref[...] = jnp.concatenate(done, axis=0).astype(BF16)


def solution(mesh):
    spec_rows = P('dp', None)
    spec_cache = P('dp', 'sp', 'tp', None)
    in_specs = (spec_rows, spec_cache, spec_cache, P('dp'), P('sp', 'tp', None), P('tp', None), P('tp', None), P(None), P(None, 'tp', None), P(None, 'tp', None), P(None, 'tp', None), P('tp', None, None), P(None), P(None, 'tp'), P('tp', None))
    out_specs = spec_rows
    vm = pl.BlockSpec(memory_space=VMEM)
    hbm = pl.BlockSpec(memory_space=pl.ANY)
    dma = pltpu.SemaphoreType.DMA
    head_weight = VMEM((HEADS, D, HEAD), BF16)
    tiles = VMEM((TILES, ROWS, 128), F32)
    by_row = VMEM((ROWS, 128), F32)

    def layer_step(hidden, k_cache, v_cache, lengths, rel_table, u_bias, w_bias, g_attn, w_query, w_key, w_value, w_out, g_mlp, w_up, w_down):
        heads_first = lambda w: jnp.transpose(w, (1, 0, 2))
        return pl.pallas_call(
            fused_kernel,
            out_shape=jax.ShapeDtypeStruct((BATCH, D), BF16),
            in_specs=[hbm] * 15,
            out_specs=vm,
            scratch_shapes=[
                pltpu.SMEM((BATCH,), jnp.int32), VMEM((BATCH, D), BF16), VMEM((D,), BF16), VMEM((D,), BF16), VMEM((HEADS, HEAD), BF16), VMEM((HEADS, HEAD), BF16),
                head_weight, VMEM((3, D, HEAD), BF16), VMEM((2 * HEADS, BATCH, HEAD), F32), VMEM((HEADS, BLK, HEAD), BF16),
                VMEM((HEADS, 128, 128), F32), VMEM((HEADS, BATCH, 128), F32), tiles, by_row, by_row, by_row,
                VMEM((RING, HEADS, BLK, HEAD), BF16), VMEM((HEADS * HEAD, D), BF16), VMEM((D, HID), BF16), VMEM((HID, D), BF16),
                tiles, tiles, tiles, tiles, tiles, VMEM((4, HEADS, BLK), F32),
                by_row, VMEM((3, ROWS, 128), F32), by_row, VMEM((4, ROWS, 128), F32),
                VMEM((GROUPS, PER, D), F32), VMEM((GROUPS, PER, D), F32), VMEM((GROUPS, PER, D), F32), VMEM((2, 8, PER, D), F32),
                VMEM((8, 1, D), F32), VMEM((8, 1, D), F32), VMEM((8, 1, D), F32), VMEM((8, 1, D), F32),
                dma((6,)), dma((2, HEADS)), dma((3,)), dma((3,)), dma((3,)), dma((RING,)), dma((3,)), dma((4,)), dma((4,)), dma((4,)), dma((4,)),
                dma((4, 3)), dma((4, 3)), dma((4, 3)), dma((4, 3)), dma((4,)), dma((4,)), dma((2, 7)), dma((2, 7)), dma((7,)), dma((7,)), dma((7,)), dma((7,)),
            ],
            compiler_params=pltpu.CompilerParams(vmem_limit_bytes=63 * 2**20, collective_id=0, has_side_effects=True),
            name="layer",
        )(
            lengths, hidden, g_attn, g_mlp, u_bias, w_bias,
            heads_first(w_query), heads_first(w_key), heads_first(w_value), heads_first(rel_table),
            jnp.transpose(k_cache, (0, 2, 1, 3)), jnp.transpose(v_cache, (0, 2, 1, 3)),
            w_out.reshape(HEADS * HEAD, D), w_up, w_down,
        )

    return jax.shard_map(layer_step, mesh=mesh, in_specs=in_specs, out_specs=out_specs, check_vma=False)
```

```python
import functools

import jax
import jax.numpy as jnp
from jax import lax
from jax.experimental import pallas as pl
from jax.experimental.pallas import tpu as pltpu
from jax.sharding import PartitionSpec as P

EPS = 1e-6
MASKED = -1e30
MESH = pl.DeviceIdType.MESH
F32 = jnp.float32
BF16 = jnp.bfloat16
VMEM = pltpu.VMEM
NT = (((1,), (1,)), ((), ()))

BATCH, HEADS, HEAD, BLK, D = 16, 6, 128, 2048, 1536
TILES = BLK // 128
GROUPS, PER = 4, 4
GROWS = HEADS * PER
ROWS = GROUPS * GROWS
RING = 8
FIRST = 6
FIRST_SEND = 9
HID = 768


def rms_norm(wide, gain):
    mean_sq = jnp.mean(wide * wide, axis=-1, keepdims=True)
    return (wide * lax.rsqrt(mean_sq + EPS) * gain).astype(BF16)


def fused_kernel(len_hbm, x_hbm, g1_hbm, g2_hbm, u_hbm, wb_hbm, wq_hbm, wk_hbm, wv_hbm, rel_hbm, k_hbm, v_hbm, wo_hbm, wu_hbm, wd_hbm,
                 out_ref,
                 len_ref, xb, g1, g2, ub, wbb, wq, wkv, kv, rel, qf, qc_ref, raw, new_score, new_value, new_prob,
                 ring, wo, wu, wd, score, rolled, from_pair, to_far, from_far, probs, stat_out, stat_in, ctx, ctx_in,
                 part_out, part_in, x1_ref, mlp_in, x1_rows, rs_out, rs_in, ag,
                 small_sem, in_sem, kv_sem, kvp_s, kvp_r, ring_sem, w_sem, pair_s, pair_r, far_s, far_r, stat_s, stat_r, ctx_s, ctx_r,
                 part_s, part_r, mlp_s, mlp_r, rs_s, rs_r, ag_s, ag_r):
    tp, sp = lax.axis_index("tp"), lax.axis_index("sp")
    me = tp * 4 + sp
    odd = lax.rem(sp, 2)
    pair = sp + 1 - 2 * odd

    small = [pltpu.make_async_copy(a, b, small_sem.at[i]) for i, (a, b) in enumerate(
        ((len_hbm, len_ref), (x_hbm, xb), (g1_hbm, g1), (g2_hbm, g2), (u_hbm, ub), (wb_hbm, wbb)))]

    def head_copy(j, h):
        a, b = ((wq_hbm, wq), (rel_hbm, rel))[j]
        return pltpu.make_async_copy(a.at[h], b.at[h], in_sem.at[j, h])

    def kv_load(src, j):
        return pltpu.make_async_copy(src.at[lax.rem(sp, 2) * 3 + j], wkv.at[j], kv_sem.at[j])

    weights = (
        pltpu.make_async_copy(wo_hbm, wo, w_sem.at[0]),
        pltpu.make_async_copy(wu_hbm.at[:, pl.ds(pl.multiple_of(sp * HID, 128), HID)], wu, w_sem.at[1]),
        pltpu.make_async_copy(wd_hbm.at[pl.ds(pl.multiple_of(sp * HID, 128), HID), :], wd, w_sem.at[2]),
    )

    def load(step, slot):
        @pl.when(step < BATCH)
        def _():
            pltpu.make_async_copy(k_hbm.at[step], ring.at[slot], ring_sem.at[slot]).start()

        @pl.when(jnp.logical_and(step >= BATCH, step < 2 * BATCH))
        def _():
            pltpu.make_async_copy(v_hbm.at[step - BATCH], ring.at[slot], ring_sem.at[slot]).start()

    for c in small:
        c.start()
    for j in range(2):
        for h in range(HEADS):
            head_copy(j, h).start()

    @pl.when(sp < 2)
    def _():
        for j in range(3):
            kv_load(wk_hbm, j).start()

    @pl.when(sp >= 2)
    def _():
        for j in range(3):
            kv_load(wv_hbm, j).start()

    for i in range(FIRST - 3):
        pltpu.make_async_copy(k_hbm.at[i], ring.at[i], ring_sem.at[i]).start()

    others = [(dt, ds) for dt in range(2) for ds in range(4) if (dt, ds) != (0, 0)]

    def peer(dt, ds):
        return lax.rem(tp + dt, 2), lax.rem(sp + ds, 4)

    def source(dt, ds):
        return lax.rem(tp + 2 - dt, 2), lax.rem(sp + 4 - ds, 4)

    barrier = pltpu.get_barrier_semaphore()
    for dt, ds in others:
        t, s = peer(dt, ds)
        pl.semaphore_signal(barrier, inc=1, device_id={"tp": t, "sp": s}, device_id_type=MESH)

    def remote(src, dst, send, recv, t, s):
        return pltpu.make_async_remote_copy(
            src_ref=src, dst_ref=dst, send_sem=send, recv_sem=recv, device_id={"tp": t, "sp": s}, device_id_type=MESH
        )

    def rows(g):
        return pl.ds(pl.multiple_of(g * GROWS, 8), GROWS)

    def pair_copy(g):
        return remote(rolled.at[:, rows(g), :], from_pair.at[:, rows(g), :], pair_s.at[g], pair_r.at[g], tp, pair)

    def far_copy(g, src=None):
        return remote((to_far if src is None else src).at[:, rows(g), :], from_far.at[:, rows(g), :], far_s.at[g], far_r.at[g], tp, 3 - sp)

    def kv_copy(ds, sending):
        t, s = peer(0, ds)
        _, fs = source(0, ds)
        part = kv.at[pl.ds((sp if sending else fs) * 3, 3)]
        return remote(part, part, kvp_s.at[ds - 1], kvp_r.at[ds - 1], t, s)

    def stat_copy(g, ds):
        t, s = peer(0, ds)
        return remote(stat_out.at[rows(g), :], stat_in.at[ds - 1, rows(g), :], stat_s.at[g, ds - 1], stat_r.at[g, ds - 1], t, s)

    def ctx_copy(g, ds, sending):
        t, s = peer(0, ds)
        _, fs = source(0, ds)
        slot = sp if sending else fs
        return remote(ctx_in.at[slot, rows(g), :], ctx_in.at[slot, rows(g), :], ctx_s.at[g, ds - 1], ctx_r.at[g, ds - 1], t, s)

    def part_copy(g):
        return remote(part_out.at[g], part_in.at[g], part_s.at[g], part_r.at[g], 1 - tp, sp)

    def mlp_copy(g, j, sending):
        t, s = peer(*others[j])
        ft, fs = source(*others[j])
        slot = me if sending else ft * 4 + fs
        return remote(mlp_in.at[g, slot], mlp_in.at[g, slot], mlp_s.at[g, j], mlp_r.at[g, j], t, s)

    def rs_copy(j, sending):
        t, s = peer(*others[j])
        ft, fs = source(*others[j])
        slot = me if sending else ft * 4 + fs
        return remote(rs_out.at[t * 4 + s], rs_in.at[slot], rs_s.at[j], rs_r.at[j], t, s)

    def ag_copy(j, sending):
        t, s = peer(*others[j])
        ft, fs = source(*others[j])
        slot = me if sending else ft * 4 + fs
        return remote(ag.at[slot], ag.at[slot], ag_s.at[j], ag_r.at[j], t, s)

    for c in small:
        c.wait()
    x = xb[...].astype(F32)
    for g in range(GROUPS):
        x1_ref[g] = x[PER * g : PER * g + PER, :]
    normed = rms_norm(x, g1[...].astype(F32).reshape(1, D))
    qf[...] = jnp.zeros_like(qf)
    for h in range(HEADS):
        head_copy(0, h).wait()
        q = jnp.dot(normed, wq[h], preferred_element_type=F32).astype(BF16).astype(F32)
        qc = (q + ub[h : h + 1, :].astype(F32)).astype(BF16).astype(F32)
        qp = (q + wbb[h : h + 1, :].astype(F32)).astype(BF16)
        qc_ref[h] = qc
        qf[h, pl.ds(h, BATCH, stride=8), :] = qc
        if h % 2 == 0:
            i = FIRST - 3 + h // 2
            pltpu.make_async_copy(k_hbm.at[i], ring.at[i], ring_sem.at[i]).start()
        head_copy(1, h).wait()
        by_dist = lax.dot_general(qp, rel[h], NT, preferred_element_type=F32)
        for c in range(TILES):
            for s in range(GROUPS):
                row = s * GROWS + h * PER
                raw[c, row : row + PER, :] = by_dist[s * PER : s * PER + PER, c * 128 : c * 128 + 128]

    def lengths_of(group, count):
        seq = lax.rem(lax.broadcasted_iota(jnp.int32, (count, 128), 0), PER)
        out = jnp.zeros((count, 128), jnp.int32) + len_ref[PER * group]
        for i in range(1, PER):
            out = jnp.where(seq == i, len_ref[PER * group + i], out)
        return out

    lane8 = lax.broadcasted_iota(jnp.int32, (8, 128), 1)

    def roll(piece):
        r = lax.rem(lengths_of(lax.div(piece, GROWS // 8), 8), BLK)
        big, small_r = lax.div(r, 128), lax.rem(r, 128)
        sl = pl.ds(pl.multiple_of(piece * 8, 8), 8)
        idx = lax.rem(small_r - lane8 + 128, 128)
        tiles = [jnp.take_along_axis(raw[(TILES - c) % TILES, sl, :], idx, axis=1) for c in range(TILES)]
        for k in range(4):
            bit = lax.rem(lax.div(big, 1 << k), 2) == 1
            tiles = [jnp.where(bit, tiles[(c - (1 << k)) % TILES], tiles[c]) for c in range(TILES)]
        low = lane8 <= small_r
        for c in range(TILES):
            rolled[c, sl, :] = jnp.where(low, tiles[c], tiles[(c + 1) % TILES])

    def content(b):
        slot = lax.rem(b, RING)
        pltpu.make_async_copy(k_hbm.at[b], ring.at[slot], ring_sem.at[slot]).wait()
        sl = pl.ds(pl.multiple_of(b * 8, 8), 8)
        total = None
        for p in range(HEADS // 2):
            keys = jnp.concatenate([ring[slot, 2 * p], ring[slot, 2 * p + 1]], axis=1)
            query = jnp.concatenate([qf[2 * p, sl, :], qf[2 * p + 1, sl, :]], axis=1).astype(BF16)
            dots = lax.dot_general(query, keys, NT, preferred_element_type=F32)
            total = dots if total is None else total + dots
        first = lax.div(b, PER) * GROWS + lax.rem(b, PER)
        for c in range(TILES):
            score[c, pl.ds(first, HEADS, stride=PER), :] = total[:HEADS, c * 128 : c * 128 + 128]
        return slot

    lane24 = lax.broadcasted_iota(jnp.int32, (GROWS, 128), 1)

    def merge(g):
        pair_copy(g).wait()
        n = lengths_of(g, GROWS)
        r = lax.rem(n, BLK)
        last = lax.div(n, BLK) == 3
        for c in range(TILES):
            mine = jnp.logical_or(jnp.logical_and(last, lane24 + 128 * c <= r), odd == 0)
            to_far[c, rows(g), :] = jnp.where(mine, rolled[c, rows(g), :], from_pair[c, rows(g), :])

    def refill(b, slot):
        @pl.when(b <= RING - FIRST - 1)
        def _():
            for k in range(2):
                nxt = FIRST + 2 * b + k
                load(nxt, lax.rem(nxt, RING))

        @pl.when(b > RING - FIRST - 1)
        def _():
            load(b + RING, slot)

    for j in range(3):
        kv_load(wk_hbm, j).wait()
        kv[sp * 3 + j] = jnp.dot(normed, wkv[j], preferred_element_type=F32).astype(BF16).astype(F32)

    def send(g):
        pair_copy(g).start()

        @pl.when(odd == 0)
        def _():
            far_copy(g, rolled).start()

    for b in range(3):
        slot = content(jnp.int32(b))
        for k in range(4):
            roll(4 * b + k)
        refill(jnp.int32(b), slot)
        if b == 0:
            pl.semaphore_wait(barrier, 7)
            for ds in range(1, 4):
                kv_copy(ds, True).start()
        send(b)
    send(3)

    def k_mid(b, _):
        slot = content(b)
        refill(b, slot)

        @pl.when(odd == 1)
        def _():
            @pl.when(b < 3 + GROUPS)
            def _():
                merge(b - 3)

            @pl.when(jnp.logical_and(b >= 4, b < 4 + GROUPS))
            def _():
                far_copy(b - 4).start()

        @pl.when(b == 9)
        def _():
            weights[0].start()

        return 0

    lax.fori_loop(3, 12, k_mid, 0)
    @pl.when(odd == 0)
    def _():
        for g in range(GROUPS):
            pair_copy(g).wait()

    def k_late(b, _):
        slot = content(b)
        refill(b, slot)
        return 0

    lax.fori_loop(12, BATCH, k_late, 0)
    for ds in range(1, 4):
        kv_copy(ds, True).wait_send()
        kv_copy(ds, False).wait_recv()
    for h in range(HEADS):
        sn = jnp.broadcast_to(jnp.sum(qc_ref[h] * kv[h], axis=1, keepdims=True), (BATCH, 128))
        for s in range(GROUPS):
            row = s * GROWS + h * PER
            new_score[row : row + PER, :] = sn[s * PER : s * PER + PER, :]
            new_value[row : row + PER, :] = kv[HEADS + h, s * PER : s * PER + PER, :]

    lane6 = lax.broadcasted_iota(jnp.int32, (HEADS, 128), 1)
    head_row = lax.broadcasted_iota(jnp.int32, (HEADS, 128), 0)

    def softmax(b):
        sl = pl.ds(lax.div(b, PER) * GROWS + lax.rem(b, PER), HEADS, stride=PER)
        n = len_ref[b]
        r = lax.rem(n, BLK)
        block = lax.div(n, BLK)
        here = n - sp * BLK
        new = new_score[sl, :]
        own_a, pair_a = block - sp == sp, block - sp == pair
        own_b, pair_b = block - sp - 1 == sp, block - sp - 1 == pair
        sc = []
        for c in range(TILES):
            pos = lane6 + 128 * c
            own, near, far = rolled[c, sl, :], from_pair[c, sl, :], from_far[c, sl, :]
            rel_a = jnp.where(own_a, own, jnp.where(pair_a, near, far))
            rel_b = jnp.where(own_b, own, jnp.where(pair_b, near, far))
            rel_c = jnp.where(pos <= r, rel_a, rel_b)
            con = jnp.where(pos == here, new, score[c, sl, :])
            sc.append(jnp.where(pos <= here, (con + rel_c) * (HEAD**-0.5), MASKED))
        top = functools.reduce(jnp.maximum, sc)
        top = jnp.max(top, axis=1, keepdims=True)
        total = jnp.zeros((HEADS, 128), F32)
        at_new = jnp.zeros((HEADS, 128), F32)
        slot = lax.rem(b, 4)
        for c in range(TILES):
            pos = lane6 + 128 * c
            w = jnp.where(pos <= here, jnp.exp(sc[c] - top), 0.0)
            total = total + w
            at_new = at_new + jnp.where(pos == here, w.astype(BF16).astype(F32), 0.0)
            probs[slot, :, c * 128 : c * 128 + 128] = jnp.where(pos == here, 0.0, w)
        total = jnp.sum(total, axis=1, keepdims=True)
        at_new = jnp.sum(at_new, axis=1, keepdims=True)
        stat_out[sl, :] = jnp.where(lane6 < 64, top, total)
        new_prob[sl, :] = jnp.broadcast_to(at_new, (HEADS, 128))

    def attend(b):
        slot = lax.rem(b + BATCH, RING)
        pltpu.make_async_copy(v_hbm.at[b], ring.at[slot], ring_sem.at[slot]).wait()
        pb = probs[lax.rem(b, 4)].astype(BF16)
        out = jnp.zeros((HEADS, 128), F32)
        for p in range(HEADS // 2):
            values = jnp.concatenate([ring[slot, 2 * p], ring[slot, 2 * p + 1]], axis=1)
            dots = jnp.dot(pb, values, preferred_element_type=F32)
            out = jnp.where(head_row == 2 * p, dots[:, :128], jnp.where(head_row == 2 * p + 1, dots[:, 128:], out))
        ctx[pl.ds(lax.div(b, PER) * GROWS + lax.rem(b, PER), HEADS, stride=PER), :] = out
        return slot

    def send_stats(g):
        for ds in range(1, 4):
            stat_copy(g, ds).start()

    def send_ctx(g):
        for ds in range(1, 4):
            stat_copy(g, ds).wait()
        mine = stat_out[rows(g), :]
        top, total = mine[:, :1], mine[:, 64:65]
        all_top = top
        for ds in range(3):
            all_top = jnp.maximum(all_top, stat_in[ds, rows(g), :][:, :1])
        all_total = total * jnp.exp(top - all_top)
        for ds in range(3):
            got = stat_in[ds, rows(g), :]
            all_total = all_total + got[:, 64:65] * jnp.exp(got[:, :1] - all_top)
        scale = jnp.exp(top - all_top) / all_total
        ctx_in[sp, rows(g), :] = (ctx[rows(g), :] + new_prob[rows(g), :] * new_value[rows(g), :]) * scale
        for ds in range(1, 4):
            ctx_copy(g, ds, True).start()

    def project(g):
        for ds in range(1, 4):
            ctx_copy(g, ds, True).wait_send()
            ctx_copy(g, ds, False).wait_recv()
        whole = (ctx_in[0, rows(g), :] + ctx_in[1, rows(g), :]) + (ctx_in[2, rows(g), :] + ctx_in[3, rows(g), :])
        lhs = jnp.concatenate([whole[h * PER : h * PER + PER, :] for h in range(HEADS)], axis=1).astype(BF16)
        part_out[g] = jnp.dot(lhs, wo[...], preferred_element_type=F32)
        part_copy(g).start()

    def middle(g):
        part_copy(g).wait()
        return (x1_ref[g] + (part_out[g] + part_in[g])).astype(BF16).astype(F32)

    def hidden_layer(x1):
        up = jnp.dot(rms_norm(x1, g2[...].astype(F32).reshape(1, D)), wu[...], preferred_element_type=F32)
        act = jax.nn.gelu(up, approximate=True).astype(BF16)
        return jnp.dot(act, wd[...], preferred_element_type=F32)

    def mlp(g):
        x1 = middle(g)
        x1_ref[g] = x1
        mlp_in[g - 2, me] = hidden_layer(x1)
        for j in range(7):
            mlp_copy(g - 2, j, True).start()

    def first_mlp():
        x1 = jnp.concatenate([middle(0), middle(1)], axis=0)
        down = hidden_layer(x1)
        for k in range(8):
            x1_rows[k] = x1[k : k + 1, :]
            rs_out[k] = down[k : k + 1, :]
        for j in range(7):
            rs_copy(j, True).start()
        rs_in[me] = rs_out[me]

    def first_sum():
        for j in range(7):
            rs_copy(j, True).wait_send()
            rs_copy(j, False).wait_recv()
        tot = rs_in[0]
        for k in range(1, 8):
            tot = tot + rs_in[k]
        ag[me] = (x1_rows[me] + tot).astype(BF16).astype(F32)
        for j in range(7):
            ag_copy(j, True).start()

    def first_finish():
        for j in range(7):
            ag_copy(j, True).wait_send()
            ag_copy(j, False).wait_recv()
        return [ag[k] for k in range(8)]

    def finish(g):
        for j in range(7):
            mlp_copy(g - 2, j, True).wait_send()
            mlp_copy(g - 2, j, False).wait_recv()
        tot = mlp_in[g - 2, 0]
        for k in range(1, 8):
            tot = tot + mlp_in[g - 2, k]
        return x1_ref[g] + tot

    far_copy(0).wait()
    softmax(0)
    softmax(1)
    softmax(2)

    def v_step(b, _):
        g, i = lax.div(b, PER), lax.rem(b, PER)

        @pl.when(jnp.logical_and(i == 1, g < GROUPS - 1))
        def _():
            far_copy(g + 1).wait()

        slot = attend(b)
        softmax(b + 3)
        load(b + BATCH + RING, slot)

        @pl.when(b == 3)
        def _():
            weights[0].wait()

        @pl.when(i == 0)
        def _():
            send_stats(g)

        @pl.when(jnp.logical_and(b >= FIRST_SEND, b < FIRST_SEND + GROUPS - 1))
        def _():
            send_ctx(b - FIRST_SEND)

        @pl.when(jnp.logical_and(b >= FIRST_SEND + 3, b < BATCH - 3))
        def _():
            project(b - FIRST_SEND - 3)

        @pl.when(b == BATCH - RING - 1)
        def _():
            weights[1].start()
            weights[2].start()

        return 0

    lax.fori_loop(0, BATCH - 3, v_step, 0)
    attend(jnp.int32(BATCH - 3))
    project(GROUPS - 3)
    attend(jnp.int32(BATCH - 2))
    project(GROUPS - 2)
    attend(jnp.int32(BATCH - 1))
    send_ctx(3)
    weights[1].wait()
    weights[2].wait()
    first_mlp()
    project(3)
    mlp(2)
    first_sum()
    mlp(3)
    done = first_finish()
    done = done + [finish(2)]
    done = done + [finish(3)]
    out_ref[...] = jnp.concatenate(done, axis=0).astype(BF16)


def solution(mesh):
    spec_rows = P('dp', None)
    spec_cache = P('dp', 'sp', 'tp', None)
    in_specs = (spec_rows, spec_cache, spec_cache, P('dp'), P('sp', 'tp', None), P('tp', None), P('tp', None), P(None), P(None, 'tp', None), P(None, 'tp', None), P(None, 'tp', None), P('tp', None, None), P(None), P(None, 'tp'), P('tp', None))
    out_specs = spec_rows
    vm = pl.BlockSpec(memory_space=VMEM)
    hbm = pl.BlockSpec(memory_space=pl.ANY)
    dma = pltpu.SemaphoreType.DMA
    head_weight = VMEM((HEADS, D, HEAD), BF16)
    tiles = VMEM((TILES, ROWS, 128), F32)
    by_row = VMEM((ROWS, 128), F32)

    def layer_step(hidden, k_cache, v_cache, lengths, rel_table, u_bias, w_bias, g_attn, w_query, w_key, w_value, w_out, g_mlp, w_up, w_down):
        heads_first = lambda w: jnp.transpose(w, (1, 0, 2))
        return pl.pallas_call(
            fused_kernel,
            out_shape=jax.ShapeDtypeStruct((BATCH, D), BF16),
            in_specs=[hbm] * 15,
            out_specs=vm,
            scratch_shapes=[
                pltpu.SMEM((BATCH,), jnp.int32), VMEM((BATCH, D), BF16), VMEM((D,), BF16), VMEM((D,), BF16), VMEM((HEADS, HEAD), BF16), VMEM((HEADS, HEAD), BF16),
                head_weight, VMEM((3, D, HEAD), BF16), VMEM((2 * HEADS, BATCH, HEAD), F32), VMEM((HEADS, BLK, HEAD), BF16),
                VMEM((HEADS, 128, 128), F32), VMEM((HEADS, BATCH, 128), F32), tiles, by_row, by_row, by_row,
                VMEM((RING, HEADS, BLK, HEAD), BF16), VMEM((HEADS * HEAD, D), BF16), VMEM((D, HID), BF16), VMEM((HID, D), BF16),
                tiles, tiles, tiles, tiles, tiles, VMEM((4, HEADS, BLK), F32),
                by_row, VMEM((3, ROWS, 128), F32), by_row, VMEM((4, ROWS, 128), F32),
                VMEM((GROUPS, PER, D), F32), VMEM((GROUPS, PER, D), F32), VMEM((GROUPS, PER, D), F32), VMEM((2, 8, PER, D), F32),
                VMEM((8, 1, D), F32), VMEM((8, 1, D), F32), VMEM((8, 1, D), F32), VMEM((8, 1, D), F32),
                dma((6,)), dma((2, HEADS)), dma((3,)), dma((3,)), dma((3,)), dma((RING,)), dma((3,)), dma((4,)), dma((4,)), dma((4,)), dma((4,)),
                dma((4, 3)), dma((4, 3)), dma((4, 3)), dma((4, 3)), dma((4,)), dma((4,)), dma((2, 7)), dma((2, 7)), dma((7,)), dma((7,)), dma((7,)), dma((7,)),
            ],
            compiler_params=pltpu.CompilerParams(vmem_limit_bytes=63 * 2**20, collective_id=0, has_side_effects=True),
            name="layer",
        )(
            lengths, hidden, g_attn, g_mlp, u_bias, w_bias,
            heads_first(w_query), heads_first(w_key), heads_first(w_value), heads_first(rel_table),
            jnp.transpose(k_cache, (0, 2, 1, 3)), jnp.transpose(v_cache, (0, 2, 1, 3)),
            w_out.reshape(HEADS * HEAD, D), w_up, w_down,
        )

    return jax.shard_map(layer_step, mesh=mesh, in_specs=in_specs, out_specs=out_specs, check_vma=False)
```
